8 devices in a mesh: rep: 1 (over z), dp: 8 (over x, y, core).
Axes of the slice: x: 2, y: 2, z: 1, core: 2. Of those that a mesh axis runs over, the one named last changes fastest.
Arguments:
- x: bfloat16 [8, 2048, 1536], P(('rep', 'dp'))
- dy: bfloat16 [8, 2048, 1536], P(('rep', 'dp'))
- w_gate: bfloat16 [2, 1536, 4224], replicated
- w_up: bfloat16 [2, 1536, 4224], replicated
- w_down: bfloat16 [2, 4224, 1536], replicated
- m_w_gate: float32 [2, 1536, 4224], P(None, 'dp')
- m_w_up: float32 [2, 1536, 4224], P(None, 'dp')
- m_w_down: float32 [2, 4224, 1536], P(None, 'dp')
- v_w_gate: float32 [2, 1536, 4224], P(None, 'dp')
- v_w_up: float32 [2, 1536, 4224], P(None, 'dp')
- v_w_down: float32 [2, 4224, 1536], P(None, 'dp')
Outputs:
- output 1: bfloat16 [2, 1536, 4224], P('rep')
- output 2: bfloat16 [2, 1536, 4224], P('rep')
- output 3: bfloat16 [2, 4224, 1536], P('rep')
- output 4: float32 [2, 1536, 4224], P('rep', 'dp')
- output 5: float32 [2, 1536, 4224], P('rep', 'dp')
- output 6: float32 [2, 4224, 1536], P('rep', 'dp')
- output 7: float32 [2, 1536, 4224], P('rep', 'dp')
- output 8: float32 [2, 1536, 4224], P('rep', 'dp')
- output 9: float32 [2, 4224, 1536], P('rep', 'dp')
All inputs are finite; a program needn't handle non-finite values.
Results may differ from the reference program's by a relative error of at most 0.022.
Values are sent between devices in bfloat16 or wider.
A program may use at most 2 GiB of HBM per device.

```python
import jax
import jax.numpy as jnp
from jax import lax

SEQUENCES = 8
TOKENS = 2048
D = 1536
FF = 4224
LAYERS = 2
NAMES = ("w_gate", "w_up", "w_down")
SHAPES = {"w_gate": (LAYERS, D, FF), "w_up": (LAYERS, D, FF), "w_down": (LAYERS, FF, D)}


def bump(key, n, height):
    away = (jnp.arange(n, dtype=jnp.int32) - jax.random.randint(key, (), 0, n, jnp.int32)) % n
    return jnp.where(away < n // 8, height, 1.0)


def together(key, own, strength):
    shared = jax.random.normal(key, own.shape[1:], jnp.float32)
    return (own + strength * shared) * lax.rsqrt(1 + strength * strength)


def setup_inputs(seed: int = 0, part: int = 0) -> dict:
    kx, kdy, ka, kb, kz, kf, kh, kl, *keys = jax.random.split(jax.random.key(seed), 8 + 3 * len(NAMES))
    kx, kdy, ka, kb = (jax.random.fold_in(k, part) for k in (kx, kdy, ka, kb))
    kw, km, kv = (keys[i::3] for i in range(3))
    shape = (SEQUENCES, TOKENS, D)
    much_x, much_dy = jax.random.uniform(kz, (2,), jnp.float32, 0.0, 1.0)
    loud = 2.0 ** jax.random.uniform(jax.random.fold_in(kz, 1), (), jnp.float32, -1.0, 2.0)
    layers = 2.0 ** jax.random.uniform(kl, (LAYERS, 1, 1), jnp.float32, -1.0, 1.0)
    x = together(ka, jax.random.normal(kx, shape, jnp.float32), much_x) * bump(kf, D, 4.0)
    dy = together(kb, jax.random.normal(kdy, shape, jnp.float32), much_dy)
    drawn = {"x": x.astype(jnp.bfloat16), "dy": (loud * dy * (SEQUENCES * TOKENS) ** -0.5).astype(jnp.bfloat16)}
    for key, name in zip(kw, NAMES, strict=True):
        w = jax.random.normal(key, SHAPES[name], jnp.float32) * SHAPES[name][1] ** -0.5
        drawn[name] = (w * {"w_gate": 1.0, "w_up": bump(kh, FF, 4.0), "w_down": layers}[name]).astype(jnp.bfloat16)
    for key, name in zip(km, NAMES, strict=True):
        drawn[f"m_{name}"] = 0.1 * jax.random.normal(key, SHAPES[name], jnp.float32)
    for key, name in zip(kv, NAMES, strict=True):
        drawn[f"v_{name}"] = jax.random.uniform(key, SHAPES[name], jnp.float32, 0.005, 0.015)
    return drawn


def matmul(a, w):
    return jnp.dot(a, w, preferred_element_type=jnp.float32).astype(jnp.bfloat16)


def normed(h):
    wide = h.astype(jnp.float32)
    scale = lax.rsqrt(jnp.mean(wide**2, -1, keepdims=True) + 1e-6)
    return (wide * scale).astype(jnp.bfloat16)


def layer(h, w):
    a = normed(h)
    gate = jnp.dot(a, w["w_gate"], preferred_element_type=jnp.float32)
    up = jnp.dot(a, w["w_up"], preferred_element_type=jnp.float32)
    return h + matmul((jax.nn.silu(gate) * up).astype(jnp.bfloat16), w["w_down"])


def adamw(w, m, v, g):
    m = 0.9 * m + 0.1 * g
    v = 0.95 * v + 0.05 * g * g
    step = m * lax.rsqrt(v + 1e-8) + 0.1 * w
    return (w - 0.02 * step).astype(jnp.bfloat16), m, v


def clipped(gradients, sum_of_squares, count):
    factor = jnp.minimum(1.0, 0.5 * lax.rsqrt(sum_of_squares / count + 1e-30))
    return [g * factor for g in gradients]


def stack(weights, h):
    return lax.scan(lambda h, w: (layer(h, w), None), h, weights)[0]


def reference(x, dy, w_gate, w_up, w_down, m_w_gate, m_w_up, m_w_down, v_w_gate, v_w_up, v_w_down):
    weights = dict(zip(NAMES, (w_gate, w_up, w_down), strict=True))

    def take(so_far, sequence):
        h, by_y = sequence
        _, back = jax.vjp(lambda w: stack(w, h), weights)
        return jax.tree.map(lambda total, term: total + term.astype(jnp.float32), so_far, back(by_y)[0]), None

    none_yet = {name: jnp.zeros(w.shape, jnp.float32) for name, w in weights.items()}
    by_weights, _ = lax.scan(take, none_yet, (x, dy))
    gradients = [by_weights[name].astype(jnp.bfloat16).astype(jnp.float32) for name in NAMES]
    gradients = clipped(gradients, sum(jnp.sum(g * g) for g in gradients), sum(g.size for g in gradients))
    new = [
        adamw(w.astype(jnp.float32), m, v, g)
        for w, m, v, g in zip((w_gate, w_up, w_down), (m_w_gate, m_w_up, m_w_down), (v_w_gate, v_w_up, v_w_down), gradients, strict=True)
    ]
    return tuple(one[which] for which in range(3) for one in new)
```

```python
import functools

import jax
import jax.numpy as jnp
from jax import lax
from jax.experimental import pallas as pl
from jax.experimental.pallas import tpu as pltpu
from jax.sharding import PartitionSpec as P


BF = jnp.bfloat16
F32 = jnp.float32
MESH = pl.DeviceIdType.MESH
TOKENS, D, FF, LAYERS = 2048, 1536, 4224, 2
BLOCK = 256
STEPS = -(-FF // BLOCK)
LAST = FF - (STEPS - 1) * BLOCK
PART = D // 8
SUB = BLOCK // 8
OWN_DOWN = FF // 8
LAST_SUB = OWN_DOWN - (STEPS - 1) * SUB
HALF = PART // 2
CHUNK = PART + HALF
COUNT = 3 * LAYERS * D * FF
VMEM_LIMIT = 67043328


ANY = pl.BlockSpec(memory_space=pl.ANY)
PIECES = [(n, l) for n in range(3) for l in range(LAYERS)]


def dot(a, b, ca, cb):
    return lax.dot_general(a, b, (((ca,), (cb,)), ((), ())), preferred_element_type=F32)


def resident(shape):
    return pl.BlockSpec(shape, lambda *_: (0,) * len(shape), pipeline_mode=pl.Buffered(1))


def cost(units, bytes_accessed):
    return pl.CostEstimate(flops=int(units * 2 * TOKENS * D * FF), bytes_accessed=int(bytes_accessed), transcendentals=0)


def normed(h):
    wide = h.astype(F32)
    scale = lax.rsqrt(jnp.mean(wide * wide, -1, keepdims=True) + 1e-6)
    return (wide * scale).astype(BF)


def forward_kernel(with_down, h_ref, wg_ref, wu_ref, *refs):
    if with_down:
        wd_ref, a_out, ht_ref, sl_ref, q_ref, next_out, a_ref, hid_ref, acc_ref, sems = refs
    else:
        a_out, ht_ref, sl_ref, q_ref, a_ref, hid_ref, sems = refs
    j = pl.program_id(0)
    keep = pltpu.make_async_copy(a_ref, a_out, sems.at[0])

    @pl.when(j == 0)
    def _():
        @pl.loop(0, TOKENS // 256)
        def _(i):
            r = pl.ds(pl.multiple_of(i * 256, 256), 256)
            a_ref[r, :] = normed(h_ref[r, :])

        keep.start()
        if with_down:
            acc_ref[...] = jnp.zeros_like(acc_ref)

    for i in range(4):
        r = slice(512 * i, 512 * i + 512)
        g = dot(a_ref[r, :], wg_ref[0], 1, 0)
        u = dot(a_ref[r, :], wu_ref[0], 1, 0)
        s = jax.nn.sigmoid(g)
        sl = g * s
        sl_ref[r, :] = sl
        q_ref[r, :] = u * (s * (1.0 + g * (1.0 - s)))
        hid = (sl * u).astype(BF)
        hid_ref[r, :] = hid
        ht_ref[:, r] = hid.T

    if with_down:

        @pl.when(j < STEPS - 1)
        def _():
            acc_ref[...] += dot(hid_ref[...], wd_ref[0], 1, 0)

        @pl.when(j == STEPS - 1)
        def _():
            acc_ref[...] += dot(hid_ref[:, :LAST], wd_ref[0, :LAST, :], 1, 0)

    @pl.when(j == STEPS - 1)
    def _():
        keep.wait()
        if with_down:

            @pl.loop(0, TOKENS // 256)
            def _(i):
                r = pl.ds(pl.multiple_of(i * 256, 256), 256)
                a_ref[r, :] = h_ref[r, :] + acc_ref[r, :].astype(BF)

            move = pltpu.make_async_copy(a_ref, next_out, sems.at[1])
            move.start()
            move.wait()


def forward(l, h, wg, wu, wd=None):
    with_down = wd is not None
    column = pl.BlockSpec((1, D, BLOCK), lambda j: (l, 0, j))
    state = jax.ShapeDtypeStruct((TOKENS, D), BF)
    wide = pl.BlockSpec((TOKENS, BLOCK), lambda j: (0, j))
    in_specs = [resident((TOKENS, D)), column, column]
    out_shape = [state, jax.ShapeDtypeStruct((FF, TOKENS), BF)] + [jax.ShapeDtypeStruct((TOKENS, FF), F32)] * 2
    out_specs = [ANY, pl.BlockSpec((BLOCK, TOKENS), lambda j: (j, 0)), wide, wide]
    scratch = [pltpu.VMEM((TOKENS, D), BF), pltpu.VMEM((TOKENS, BLOCK), BF)]
    args = [h, wg, wu]
    if with_down:
        in_specs.append(pl.BlockSpec((1, BLOCK, D), lambda j: (l, j, 0)))
        out_shape.append(state)
        out_specs.append(ANY)
        scratch.append(pltpu.VMEM((TOKENS, D), F32))
        args.append(wd)
    return pl.pallas_call(
        functools.partial(forward_kernel, with_down),
        grid=(STEPS,),
        in_specs=in_specs,
        out_specs=out_specs,
        out_shape=out_shape,
        scratch_shapes=scratch + [pltpu.SemaphoreType.DMA((2,))],
        compiler_params=pltpu.CompilerParams(vmem_limit_bytes=VMEM_LIMIT),
        cost_estimate=cost(3 if with_down else 2, 130e6),
    )(*args)


class Lags:
    def __init__(self, first, second, third, b, e):
        self.first, self.second, self.third = first, second, third
        self.s = third + 1
        self.a = first + third + 2 * (first == 0)
        self.b, self.e = b, e
        self.c = second + third - 2 * first
        self.d = 2 * (third - second)


def backward_kernel(lags, with_da, a_ref, dy_ref, wd_ref, sl_ref, q_ref, ht_ref, *refs):
    if with_da:
        wg_ref, wu_ref, *refs = refs
    g_gate, g_up, g_down, sq_ref, *refs = refs
    if with_da:
        da_out, acc_ref, *refs = refs
    dgu_ref, s_ref, a2_ref, bx, by, cx, cy, ex, ey, dx, dy2, og, ou, od, *sems = refs
    s_send, a_recv, bx_send, by_send, cx_recv, cy_recv, ex_send, ey_send, dx_recv, dy_recv, out_sem, da_sem = sems
    j = pl.program_id(0)
    me = lax.axis_index("dp")
    x, y, c = lax.div(me, 4), lax.rem(lax.div(me, 2), 2), lax.rem(me, 2)
    to_core, to_x, to_y = ({"dp": me + k * (1 - 2 * t)} for k, t in ((1, c), (4, x), (2, y)))

    def remote(src, dst, send, recv, to):
        return pltpu.make_async_remote_copy(src_ref=src, dst_ref=dst, send_sem=send, recv_sem=recv, device_id=to, device_id_type=MESH)

    def pair(i):
        s, a = lax.rem(i, lags.s), lax.rem(i, lags.a)
        return remote(s_ref.at[s, :, :, :, 1 - c], a2_ref.at[a], s_send.at[s], a_recv.at[a], to_core)

    def first(i):
        b, k = lax.rem(i, lags.b), lax.rem(i, lags.c)
        return (
            remote(bx.at[b], cx.at[k], bx_send.at[b], cx_recv.at[k], to_x),
            remote(by.at[b], cy.at[k], by_send.at[b], cy_recv.at[k], to_y),
        )

    def second(i):
        e, k = lax.rem(i, lags.e), lax.rem(i, lags.d)
        return (
            remote(ex.at[e], dx.at[k], ex_send.at[e], dx_recv.at[k], to_x),
            remote(ey.at[e], dy2.at[k], ey_send.at[e], dy_recv.at[k], to_y),
        )

    def outs(i, last):
        o = lax.rem(i, 2)
        if last:
            wide, deep = pl.ds((STEPS - 1) * BLOCK, LAST), pl.ds((STEPS - 1) * SUB, LAST_SUB)
            srcs = og.at[o, :, pl.ds(0, LAST)], ou.at[o, :, pl.ds(0, LAST)], od.at[o, pl.ds(0, LAST_SUB)]
        else:
            wide, deep = pl.ds(pl.multiple_of(i * BLOCK, BLOCK), BLOCK), pl.ds(pl.multiple_of(i * SUB, SUB), SUB)
            srcs = og.at[o], ou.at[o], od.at[o]
        dsts = g_gate.at[:, wide], g_up.at[:, wide], g_down.at[deep]
        return [pltpu.make_async_copy(s, d, out_sem.at[o, n]) for n, (s, d) in enumerate(zip(srcs, dsts))]

    def total(*terms):
        return functools.reduce(lambda p, q: p + q, [t.astype(F32) for t in terms])

    def take_first(i):
        pair(i).wait()
        s, a, b = lax.rem(i, lags.s), lax.rem(i, lags.a), lax.rem(i, lags.b)

        @pl.when(i >= lags.b)
        def _():
            for copy in first(i - lags.b):
                copy.wait_send()

        for t in range(2):
            bx[b, t, :PART] = total(s_ref[s, 0, 1 - x, t, c], a2_ref[a, 0, 1 - x, t]).astype(BF)
            bx[b, t, PART:] = total(s_ref[s, 2, 1 - x, t, c, :HALF], a2_ref[a, 2, 1 - x, t, :HALF]).astype(BF)
            by[b, t, :PART] = total(s_ref[s, 1, t, 1 - y, c], a2_ref[a, 1, t, 1 - y]).astype(BF)
            by[b, t, PART:] = total(s_ref[s, 2, t, 1 - y, c, HALF:], a2_ref[a, 2, t, 1 - y, HALF:]).astype(BF)
        for copy in first(i):
            copy.start()

    def take_second(i):
        for copy in first(i):
            copy.wait_recv()
        s, a, k, e = lax.rem(i, lags.s), lax.rem(i, lags.a), lax.rem(i, lags.c), lax.rem(i, lags.e)

        @pl.when(i >= lags.e)
        def _():
            for copy in second(i - lags.e):
                copy.wait_send()

        ey[e, :PART] = total(s_ref[s, 0, x, 1 - y, c], a2_ref[a, 0, x, 1 - y], cx[k, 1 - y, :PART]).astype(BF)
        ey[e, PART:] = total(s_ref[s, 2, x, 1 - y, c, :HALF], a2_ref[a, 2, x, 1 - y, :HALF], cx[k, 1 - y, PART:]).astype(BF)
        ex[e, :PART] = total(s_ref[s, 1, 1 - x, y, c], a2_ref[a, 1, 1 - x, y], cy[k, 1 - x, :PART]).astype(BF)
        ex[e, PART:] = total(s_ref[s, 2, 1 - x, y, c, HALF:], a2_ref[a, 2, 1 - x, y, HALF:], cy[k, 1 - x, PART:]).astype(BF)
        for copy in second(i):
            copy.start()

    def take_third(i):
        for copy in second(i):
            copy.wait_recv()
        s, a, k, d, o = (lax.rem(i, n) for n in (lags.s, lags.a, lags.c, lags.d, 2))

        @pl.when(i >= 2)
        def _():
            for copy in outs(i - 2, False):
                copy.wait()

        gate = total(s_ref[s, 0, x, y, c], a2_ref[a, 0, x, y], cx[k, y, :PART], dy2[d, :PART]).astype(BF)
        up = total(s_ref[s, 1, x, y, c], a2_ref[a, 1, x, y], cy[k, x, :PART], dx[d, :PART]).astype(BF)
        og[o] = gate
        ou[o] = up
        low = total(s_ref[s, 2, x, y, c, :HALF], a2_ref[a, 2, x, y, :HALF], cx[k, y, PART:], dy2[d, PART:]).astype(BF)
        high = total(s_ref[s, 2, x, y, c, HALF:], a2_ref[a, 2, x, y, HALF:], cy[k, x, PART:], dx[d, PART:]).astype(BF)
        downs = [half[SUB * n : SUB * n + SUB] for half in (low, high) for n in range(HALF // SUB)]
        for n, one in enumerate(downs):
            od[o, :, BLOCK * n : BLOCK * n + BLOCK] = one

        def squares(t):
            wide = t.astype(F32)
            return jnp.sum((wide * wide).reshape(-1, 8, t.shape[-1]), 0)

        @pl.when(i < STEPS - 1)
        def _():
            sq_ref[...] += squares(gate) + squares(up) + squares(low) + squares(high)
            for copy in outs(i, False):
                copy.start()

        @pl.when(i == STEPS - 1)
        def _():
            sq_ref[:, :LAST] += squares(gate[:, :LAST]) + squares(up[:, :LAST])
            sq_ref[...] += sum(squares(one[:LAST_SUB]) for one in downs)
            for copy in outs(i, True):
                copy.start()

    @pl.when(j == 0)
    def _():
        sq_ref[...] = jnp.zeros_like(sq_ref)
        if with_da:
            acc_ref[...] = jnp.zeros_like(acc_ref)
        barrier = pltpu.get_barrier_semaphore()
        for to in (to_core, to_x, to_y):
            pl.semaphore_signal(barrier, inc=1, device_id=to, device_id_type=MESH)
        pl.semaphore_wait(barrier, 3)

    @pl.when(j < STEPS)
    def _():
        s = lax.rem(j, lags.s)
        for i in range(4):
            r = slice(512 * i, 512 * i + 512)
            dh = dot(dy_ref[r, :], wd_ref[0], 1, 1).astype(BF).astype(F32)
            dgu_ref[r, :BLOCK] = (dh * q_ref[r, :]).astype(BF)
            dgu_ref[r, BLOCK:] = (dh * sl_ref[r, :]).astype(BF)
        for h in range(2):
            gu = dot(a_ref[:, D // 2 * h : D // 2 * (h + 1)], dgu_ref[...], 0, 0)
            for o in range(4):
                for t in range(2):
                    s_ref[s, t, h, o // 2, o % 2] = gu[PART * o : PART * o + PART, BLOCK * t : BLOCK * t + BLOCK].astype(BF)
        for h in range(2):
            down = dot(ht_ref[...].reshape(BLOCK, TOKENS), dy_ref[:, D // 2 * h : D // 2 * (h + 1)], 1, 0)
            for o in range(8):
                for n in range(3):
                    s_ref[s, 2, o // 4, o // 2 % 2, o % 2, SUB * (3 * h + n) : SUB * (3 * h + n + 1)] = down[
                        SUB * o : SUB * o + SUB, BLOCK * n : BLOCK * n + BLOCK
                    ].astype(BF)
        if lags.first == 0:
            pair(j).start()

    if with_da:

        def add_da(width):
            for i in range(4):
                r = slice(512 * i, 512 * i + 512)
                acc_ref[r, :] += dot(dgu_ref[r, :width], wg_ref[0, :, :width], 1, 1) + dot(
                    dgu_ref[r, BLOCK : BLOCK + width], wu_ref[0, :, :width], 1, 1
                )

        pl.when(j < STEPS - 1)(functools.partial(add_da, BLOCK))
        pl.when(j == STEPS - 1)(functools.partial(add_da, LAST))

    pl.when((j >= lags.third) & (j < STEPS + lags.third))(lambda: take_third(j - lags.third))
    pl.when((j >= lags.second) & (j < STEPS + lags.second))(lambda: take_second(j - lags.second))
    pl.when((j >= lags.first) & (j < STEPS + lags.first))(lambda: take_first(j - lags.first))
    if lags.first > 0:
        pl.when(j < STEPS)(lambda: pair(j).start())

    if with_da:

        @pl.when(j == STEPS)
        def _():
            for n in range(3):
                wide = slice(512 * n, 512 * n + 512)
                dgu_ref[...] = acc_ref[:, wide].astype(BF)
                move = pltpu.make_async_copy(dgu_ref, da_out.at[:, pl.ds(512 * n, 512)], da_sem)
                move.start()
                move.wait()

    @pl.when(j == STEPS + lags.third - 1)
    def _():
        for i in range(STEPS - lags.b, STEPS):
            for copy in first(jnp.int32(i)):
                copy.wait_send()
        for i in range(STEPS - lags.e, STEPS):
            for copy in second(jnp.int32(i)):
                copy.wait_send()
        for i in range(STEPS - 2, STEPS):
            for copy in outs(jnp.int32(i), i == STEPS - 1):
                copy.wait()


def backward(l, lags, a, dy, wd, sl, q, ht, wg=None, wu=None):
    with_da = wg is not None
    at = lambda j: jnp.minimum(j, STEPS - 1)
    wide = pl.BlockSpec((TOKENS, BLOCK), lambda j: (0, at(j)))
    in_specs = [
        resident((TOKENS, D)),
        resident((TOKENS, D)),
        pl.BlockSpec((1, BLOCK, D), lambda j: (l, at(j), 0)),
        wide,
        wide,
        pl.BlockSpec((8, SUB, TOKENS), lambda j: (0, at(j), 0)),
    ]
    args = [a, dy, wd, sl, q, ht.reshape(8, OWN_DOWN, TOKENS)]
    out_shape = [jax.ShapeDtypeStruct((PART, FF), BF)] * 2 + [jax.ShapeDtypeStruct((OWN_DOWN, D), BF), jax.ShapeDtypeStruct((8, BLOCK), F32)]
    out_specs = [ANY] * 3 + [pl.BlockSpec((8, BLOCK), lambda j: (0, 0))]
    scratch = []
    if with_da:
        column = pl.BlockSpec((1, D, BLOCK), lambda j: (l, 0, at(j)))
        in_specs += [column, column]
        args += [wg, wu]
        out_shape.append(jax.ShapeDtypeStruct((TOKENS, D), BF))
        out_specs.append(ANY)
        scratch.append(pltpu.VMEM((TOKENS, D), F32))
    piece = (PART, BLOCK)
    scratch += [
        pltpu.VMEM((TOKENS, 2 * BLOCK), BF),
        pltpu.VMEM((lags.s, 3, 2, 2, 2) + piece, BF),
        pltpu.VMEM((lags.a, 3, 2, 2) + piece, BF),
        *[pltpu.VMEM((lags.b, 2, CHUNK, BLOCK), BF)] * 2,
        *[pltpu.VMEM((lags.c, 2, CHUNK, BLOCK), BF)] * 2,
        *[pltpu.VMEM((lags.e, CHUNK, BLOCK), BF)] * 2,
        *[pltpu.VMEM((lags.d, CHUNK, BLOCK), BF)] * 2,
        *[pltpu.VMEM((2,) + piece, BF)] * 2,
        pltpu.VMEM((2, SUB, D), BF),
    ]
    counts = (lags.s, lags.a, lags.b, lags.b, lags.c, lags.c, lags.e, lags.e, lags.d, lags.d)
    scratch += [pltpu.SemaphoreType.DMA((n,)) for n in counts]
    scratch += [pltpu.SemaphoreType.DMA((2, 3)), pltpu.SemaphoreType.DMA]
    return pl.pallas_call(
        functools.partial(backward_kernel, lags, with_da),
        grid=(STEPS + lags.third,),
        in_specs=in_specs,
        out_specs=out_specs,
        out_shape=out_shape,
        scratch_shapes=scratch,
        compiler_params=pltpu.CompilerParams(vmem_limit_bytes=VMEM_LIMIT, collective_id=l, has_side_effects=True),
        cost_estimate=cost(6 if with_da else 4, 150e6),
    )(*args)


def factor_kernel(p_ref, q_ref, f_ref, buf, send, recv):
    me = lax.axis_index("dp")
    barrier = pltpu.get_barrier_semaphore()
    peers = [lax.rem(me + k, 8) for k in range(1, 8)]
    for peer in peers:
        pl.semaphore_signal(barrier, inc=1, device_id={"dp": peer}, device_id_type=MESH)
    both = p_ref[...] + q_ref[...]
    buf[me] = both[:, :128] + both[:, 128:]
    pl.semaphore_wait(barrier, 7)

    def copy(k):
        return pltpu.make_async_remote_copy(
            src_ref=buf.at[me], dst_ref=buf.at[me], send_sem=send.at[k], recv_sem=recv.at[k], device_id={"dp": peers[k]}, device_id_type=MESH
        )

    for k in range(7):
        copy(k).start()
    for k in range(7):
        copy(k).wait()
    every = buf[0]
    for k in range(1, 8):
        every = every + buf[k]
    total = jnp.sum(jnp.sum(every, axis=1, keepdims=True), axis=0, keepdims=True)
    f_ref[...] = jnp.broadcast_to(jnp.minimum(1.0, 0.5 * lax.rsqrt(total / COUNT + 1e-30)), (8, 128))


def clip_factor(p, q):
    return pl.pallas_call(
        factor_kernel,
        in_specs=[pl.BlockSpec(memory_space=pltpu.VMEM)] * 2,
        out_specs=pl.BlockSpec(memory_space=pltpu.VMEM),
        out_shape=jax.ShapeDtypeStruct((8, 128), F32),
        scratch_shapes=[pltpu.VMEM((8, 8, 128), F32), pltpu.SemaphoreType.DMA((7,)), pltpu.SemaphoreType.DMA((7,))],
        compiler_params=pltpu.CompilerParams(collective_id=2, has_side_effects=True),
        name="factor",
    )(p, q)


def adamw_kernel(at_ref, f_ref, g_ref, w_ref, m_ref, v_ref, *refs):
    nw_ref, nm_ref, nv_ref = refs[-3:]
    g = g_ref[...].astype(F32) * f_ref[0:1, 0:1]
    w = w_ref[0].astype(F32)
    m = 0.9 * m_ref[0] + 0.1 * g
    v = 0.95 * v_ref[0] + 0.05 * g * g
    nm_ref[0] = m
    nv_ref[0] = v
    nw_ref[...] = (w - 0.02 * (m * lax.rsqrt(v + 1e-8) + 0.1 * w)).astype(BF)


def adamw(l, at, factor, g, w, m, v, so_far=None):
    rows, columns = g.shape
    deep = rows // 3
    moment = pl.BlockSpec((1, deep, columns), lambda i, at: (l, i, 0))
    flat = pl.BlockSpec((deep, columns), lambda i, at: (i, 0))
    in_specs = [
        pl.BlockSpec((8, 128), lambda i, at: (0, 0)),
        flat,
        pl.BlockSpec((1, deep, columns), lambda i, at: (l, 3 * at[0] + i, 0)),
        moment,
        moment,
    ]
    args = [factor, g, w, m, v]
    aliases = {}
    if so_far is not None:
        in_specs += [ANY, ANY]
        args += so_far
        aliases = {6: 1, 7: 2}
    return pl.pallas_call(
        adamw_kernel,
        grid_spec=pltpu.PrefetchScalarGridSpec(num_scalar_prefetch=1, grid=(3,), in_specs=in_specs, out_specs=[flat, moment, moment]),
        out_shape=[jax.ShapeDtypeStruct(g.shape, BF)] + [jax.ShapeDtypeStruct(m.shape, F32)] * 2,
        input_output_aliases=aliases,
        compiler_params=pltpu.CompilerParams(vmem_limit_bytes=48 << 20),
        cost_estimate=cost(0.1, 22 * rows * columns),
    )(at, *args)


def place_kernel(n, owners_ref, *refs):
    out_ref = refs[-1]
    s = pl.program_id(0)
    for k in range(n):

        @pl.when(s == k)
        def _():
            out_ref[0] = refs[k][...]


def place(l, owners, pieces, so_far):
    n = len(pieces)
    rows, columns = pieces[0].shape
    cut = 1 if n > 1 else 3
    deep = rows // cut
    in_specs = [
        pl.BlockSpec((deep, columns), lambda s, i, own, k=k: (jnp.where(s == k, i, jnp.where(s < k, 0, cut - 1)), 0)) for k in range(n)
    ]
    args = list(pieces)
    aliases = {}
    if so_far is not None:
        in_specs.append(ANY)
        args.append(so_far)
        aliases = {n + 1: 0}
    return pl.pallas_call(
        functools.partial(place_kernel, n),
        grid_spec=pltpu.PrefetchScalarGridSpec(
            num_scalar_prefetch=1,
            grid=(n, cut),
            in_specs=in_specs,
            out_specs=pl.BlockSpec((1, deep, columns), lambda s, i, own: (l, cut * own[s] + i, 0)),
        ),
        out_shape=jax.ShapeDtypeStruct((LAYERS, 8 * rows, columns), BF),
        input_output_aliases=aliases,
        compiler_params=pltpu.CompilerParams(vmem_limit_bytes=48 << 20),
        cost_estimate=cost(0.1 * n, 4 * n * rows * columns),
    )(owners, *args)


def solution(mesh):
    def swap(t, mask):
        return lax.ppermute(t, "dp", [(i, i ^ mask) for i in range(8)])

    def step(x, dy, wg, wu, wd, mg, mu, md, vg, vu, vd):
        x, dy = x[0], dy[0]
        me = lax.axis_index("dp")
        a0, ht0, sl0, q0, h1 = forward(0, x, wg, wu, wd)
        a1, ht1, sl1, q1 = forward(1, h1, wg, wu)
        g1 = backward(1, Lags(0, 1, 2, 2, 2), a1, dy, wd, sl1, q1, ht1, wg, wu)
        _, back = jax.vjp(normed, h1)
        dh1 = dy + back(g1[4])[0]
        g0 = backward(0, Lags(1, 3, 4, 3, 3), a0, dh1, wd, sl0, q0, ht0)
        factor = clip_factor(g0[3], g1[3])
        at = me[None].astype(jnp.int32)
        owners = {k: (me ^ k).astype(jnp.int32) for k in range(8)}
        mats = ((wg, mg, vg), (wu, mu, vu), (wd, md, vd))
        moments, whole = [None] * 3, [None] * 3

        def put(n, l, have, group):
            whole[n] = place(l, jnp.stack([owners[k] for k in group]), [have[k] for k in group], whole[n])

        everything = []
        for number, (n, l) in enumerate(PIECES):
            have = {}
            everything.append(have)
            have[0], *moments[n] = adamw(l, at, factor, (g0, g1)[l][n], *mats[n], moments[n])
            have[4] = swap(have[0], 4)
            have[2] = swap(have[0], 2)
            have[6] = swap(have[4], 2) if number % 2 else swap(have[2], 4)
            for k in (0, 4, 2, 6):
                have[k + 1] = swap(have[k], 1)
            put(n, l, have, (0, 1))
            put(n, l, have, (4, 2, 5, 3))
        for number, (n, l) in enumerate(PIECES):
            put(n, l, everything[number], (6,))
            put(n, l, everything[number], (7,))
        new_w, new_m, new_v = whole, [m[0] for m in moments], [m[1] for m in moments]
        return tuple(new_w + new_m + new_v)

    whole, rows = P(None, None, None), P(None, "dp", None)
    return jax.shard_map(
        step,
        mesh=mesh,
        in_specs=(P(("rep", "dp")),) * 2 + (whole,) * 3 + (rows,) * 6,
        out_specs=(P("rep"),) * 3 + (P("rep", "dp"),) * 6,
        check_vma=False,
    )
```

```python
import functools

import jax
import jax.numpy as jnp
from jax import lax
from jax.experimental import pallas as pl
from jax.experimental.pallas import tpu as pltpu
from jax.sharding import PartitionSpec as P


BF = jnp.bfloat16
F32 = jnp.float32
MESH = pl.DeviceIdType.MESH
TOKENS, D, FF, LAYERS = 2048, 1536, 4224, 2
BLOCK = 256
STEPS = -(-FF // BLOCK)
LAST = FF - (STEPS - 1) * BLOCK
PART = D // 8
SUB = BLOCK // 8
OWN_DOWN = FF // 8
LAST_SUB = OWN_DOWN - (STEPS - 1) * SUB
HALF = PART // 2
CHUNK = PART + HALF
COUNT = 3 * LAYERS * D * FF
VMEM_LIMIT = 67043328


ANY = pl.BlockSpec(memory_space=pl.ANY)
GROUPS = {"own": (0, 1), "near": (4, 2, 5, 3), "across": (6,), "last": (7,)}


def dot(a, b, ca, cb):
    return lax.dot_general(a, b, (((ca,), (cb,)), ((), ())), preferred_element_type=F32)


def resident(shape):
    return pl.BlockSpec(shape, lambda *_: (0,) * len(shape), pipeline_mode=pl.Buffered(1))


def cost(units, bytes_accessed):
    return pl.CostEstimate(flops=int(units * 2 * TOKENS * D * FF), bytes_accessed=int(bytes_accessed), transcendentals=0)


def normed(h):
    wide = h.astype(F32)
    scale = lax.rsqrt(jnp.mean(wide * wide, -1, keepdims=True) + 1e-6)
    return (wide * scale).astype(BF)


class Weights:
    def __init__(self, l, wg, wu, wd, gu_ref, down_ref, sems):
        self.l, self.wg, self.wu, self.wd, self.gu_ref, self.down_ref, self.sems = l, wg, wu, wd, gu_ref, down_ref, sems

    def copies(self, j, last):
        slot = lax.rem(j, 2)
        width = LAST if last else BLOCK
        start = (STEPS - 1) * BLOCK if last else pl.multiple_of(j * BLOCK, BLOCK)
        columns = pl.ds(start, width)
        pairs = [
            (self.wg.at[self.l, :, columns], self.gu_ref.at[slot, :, pl.ds(0, width)]),
            (self.wu.at[self.l, :, columns], self.gu_ref.at[slot, :, pl.ds(BLOCK, width)]),
        ]
        if self.wd is not None:
            pairs.append((self.wd.at[self.l, columns], self.down_ref.at[slot, pl.ds(0, width)]))
        return [pltpu.make_async_copy(src, dst, self.sems.at[slot, n]) for n, (src, dst) in enumerate(pairs)]

    def each(self, j, act):
        @pl.when(j < STEPS - 1)
        def _():
            for copy in self.copies(j, False):
                act(copy)

        @pl.when(j == STEPS - 1)
        def _():
            for copy in self.copies(j, True):
                act(copy)

    def start(self, j):
        self.each(j, lambda copy: copy.start())

    def wait(self, j):
        self.each(j, lambda copy: copy.wait())


def forward_kernel(l, with_down, h_ref, wg, wu, *refs):
    if with_down:
        wd, a_out, ht_ref, sl_ref, q_ref, next_out, a_ref, gu_ref, w_sems, sems, hid_ref, acc_ref, down_ref = refs
    else:
        a_out, ht_ref, sl_ref, q_ref, a_ref, gu_ref, w_sems, sems = refs
        wd = hid_ref = down_ref = None
    j = pl.program_id(0)
    weights = Weights(l, wg, wu, wd, gu_ref, down_ref, w_sems)
    keep = pltpu.make_async_copy(a_ref, a_out, sems.at[0])

    @pl.when(j == 0)
    def _():
        weights.start(j)

        @pl.loop(0, TOKENS // 256)
        def _(i):
            r = pl.ds(pl.multiple_of(i * 256, 256), 256)
            a_ref[r, :] = normed(h_ref[r, :])
            if with_down:
                acc_ref[r, :] = jnp.zeros((256, D), F32)

        keep.start()

    weights.start(j + 1)
    weights.wait(j)
    slot = lax.rem(j, 2)
    for i in range(8):
        r = slice(256 * i, 256 * i + 256)
        gu = dot(a_ref[r, :], gu_ref[slot], 1, 0)
        g, u = gu[:, :BLOCK], gu[:, BLOCK:]
        s = jax.nn.sigmoid(g)
        sl = g * s
        sl_ref[r, :] = sl
        q_ref[r, :] = u * (s * (1.0 + g * (1.0 - s)))
        hid = (sl * u).astype(BF)
        if with_down:
            hid_ref[r, :] = hid
        ht_ref[:, r] = hid.T

    if with_down:

        @pl.when(j == STEPS - 1)
        def _():
            hid_ref[:, LAST:] = jnp.zeros((TOKENS, BLOCK - LAST), BF)

        acc_ref[...] += dot(hid_ref[...], down_ref[slot], 1, 0)

    @pl.when(j == STEPS - 1)
    def _():
        keep.wait()
        if with_down:

            @pl.loop(0, TOKENS // 256)
            def _(i):
                r = pl.ds(pl.multiple_of(i * 256, 256), 256)
                a_ref[r, :] = h_ref[r, :] + acc_ref[r, :].astype(BF)

            move = pltpu.make_async_copy(a_ref, next_out, sems.at[1])
            move.start()
            move.wait()


def forward(l, h, wg, wu, wd=None):
    with_down = wd is not None
    state = jax.ShapeDtypeStruct((TOKENS, D), BF)
    wide = pl.BlockSpec((TOKENS, BLOCK), lambda j: (0, j))
    in_specs = [resident((TOKENS, D)), ANY, ANY]
    out_shape = [state, jax.ShapeDtypeStruct((FF, TOKENS), BF)] + [jax.ShapeDtypeStruct((TOKENS, FF), F32)] * 2
    out_specs = [ANY, pl.BlockSpec((BLOCK, TOKENS), lambda j: (j, 0)), wide, wide]
    scratch = [
        pltpu.VMEM((TOKENS, D), BF),
        pltpu.VMEM((2, D, 2 * BLOCK), BF),
        pltpu.SemaphoreType.DMA((2, 3)),
        pltpu.SemaphoreType.DMA((2,)),
    ]
    args = [h, wg, wu]
    if with_down:
        in_specs.append(ANY)
        out_shape.append(state)
        out_specs.append(ANY)
        scratch += [pltpu.VMEM((TOKENS, BLOCK), BF), pltpu.VMEM((TOKENS, D), F32), pltpu.VMEM((2, BLOCK, D), BF)]
        args.append(wd)
    return pl.pallas_call(
        functools.partial(forward_kernel, l, with_down),
        grid=(STEPS,),
        in_specs=in_specs,
        out_specs=out_specs,
        out_shape=out_shape,
        scratch_shapes=scratch,
        compiler_params=pltpu.CompilerParams(vmem_limit_bytes=VMEM_LIMIT),
        cost_estimate=cost(3 if with_down else 2, 130e6),
    )(*args)


class Lags:
    def __init__(self, second, third, b, e):
        self.second, self.third, self.b, self.e = second, third, b, e
        self.s = third + 1
        self.a = third + 2
        self.c = second + third
        self.d = 2 * (third - second)


def backward_kernel(l, lags, a_in, dy_ref, wd_ref, sl_ref, q_ref, ht_ref, *refs):
    with_da = l == 1
    if with_da:
        wg, wu, h_in, g_gate, g_up, g_down, sq_ref, dh_out, acc_ref, gu_ref, w_sems, *refs = refs
        weights = Weights(l, wg, wu, None, gu_ref, None, w_sems)
    else:
        other_ref, g_gate, g_up, g_down, f_ref, sq_ref, every_ref, f_send, f_recv, *refs = refs
    a_ref, dgu_ref, s_ref, a2_ref, bx, by, cx, cy, ex, ey, dx, dy2, og, ou, od, *sems = refs
    s_send, a_recv, bx_send, by_send, cx_recv, cy_recv, ex_send, ey_send, dx_recv, dy_recv, out_sem, a_sem = sems
    j = pl.program_id(0)
    me = lax.axis_index("dp")
    x, y, c = lax.div(me, 4), lax.rem(lax.div(me, 2), 2), lax.rem(me, 2)
    to_core, to_x, to_y = ({"dp": me + k * (1 - 2 * t)} for k, t in ((1, c), (4, x), (2, y)))
    others = [{"dp": lax.rem(me + k, 8)} for k in range(1, 8)]

    def remote(src, dst, send, recv, to):
        return pltpu.make_async_remote_copy(src_ref=src, dst_ref=dst, send_sem=send, recv_sem=recv, device_id=to, device_id_type=MESH)

    def columns(last):
        return pl.ds(0, LAST if last else BLOCK)

    def pair(i, last, which=(0, 1)):
        s, a, w = lax.rem(i, lags.s), lax.rem(i, lags.a), columns(last)
        return [
            remote(s_ref.at[s, n, :, :, 1 - c, :, w], a2_ref.at[a, n, :, :, :, w], s_send.at[s, k], a_recv.at[a, k], to_core)
            for k, n in ((k, (pl.ds(0, 2), pl.ds(2, 1))[k]) for k in which)
        ]

    def first(i, last):
        b, k, w = lax.rem(i, lags.b), lax.rem(i, lags.c), columns(last)
        return [
            remote(bx.at[b, :, :, w], cx.at[k, :, :, w], bx_send.at[b], cx_recv.at[k], to_x),
            remote(by.at[b, :, :, w], cy.at[k, :, :, w], by_send.at[b], cy_recv.at[k], to_y),
        ]

    def second(i, last):
        e, k, w = lax.rem(i, lags.e), lax.rem(i, lags.d), columns(last)
        return [
            remote(ex.at[e, :, w], dx.at[k, :, w], ex_send.at[e], dx_recv.at[k], to_x),
            remote(ey.at[e, :, w], dy2.at[k, :, w], ey_send.at[e], dy_recv.at[k], to_y),
        ]

    def outs(i, last):
        o = lax.rem(i, 2)
        if last:
            wide, deep = pl.ds((STEPS - 1) * BLOCK, LAST), pl.ds((STEPS - 1) * SUB, LAST_SUB)
            srcs = og.at[o, :, pl.ds(0, LAST)], ou.at[o, :, pl.ds(0, LAST)], od.at[o, pl.ds(0, LAST_SUB)]
        else:
            wide, deep = pl.ds(pl.multiple_of(i * BLOCK, BLOCK), BLOCK), pl.ds(pl.multiple_of(i * SUB, SUB), SUB)
            srcs = og.at[o], ou.at[o], od.at[o]
        dsts = g_gate.at[:, wide], g_up.at[:, wide], g_down.at[deep]
        return [pltpu.make_async_copy(s, d, out_sem.at[o, n]) for n, (s, d) in enumerate(zip(srcs, dsts))]

    def each(i, copies, act):
        @pl.when(i < STEPS - 1)
        def _():
            for copy in copies(i, False):
                act(copy)

        @pl.when(i == STEPS - 1)
        def _():
            for copy in copies(i, True):
                act(copy)

    def start(copy):
        copy.start()

    def total(*terms):
        return functools.reduce(lambda p, q: p + q, [t.astype(F32) for t in terms])

    def take_first(i):
        each(i, pair, lambda copy: copy.wait())
        s, a, b = lax.rem(i, lags.s), lax.rem(i, lags.a), lax.rem(i, lags.b)

        @pl.when(i >= lags.b)
        def _():
            for copy in first(i - lags.b, False):
                copy.wait_send()

        for t in range(2):
            bx[b, t, :PART] = total(s_ref[s, 0, 1 - x, t, c], a2_ref[a, 0, 1 - x, t]).astype(BF)
            bx[b, t, PART:] = total(s_ref[s, 2, 1 - x, t, c, :HALF], a2_ref[a, 2, 1 - x, t, :HALF]).astype(BF)
            by[b, t, :PART] = total(s_ref[s, 1, t, 1 - y, c], a2_ref[a, 1, t, 1 - y]).astype(BF)
            by[b, t, PART:] = total(s_ref[s, 2, t, 1 - y, c, HALF:], a2_ref[a, 2, t, 1 - y, HALF:]).astype(BF)
        each(i, first, start)

    def take_second(i):
        each(i, first, lambda copy: copy.wait_recv())
        s, a, k, e = lax.rem(i, lags.s), lax.rem(i, lags.a), lax.rem(i, lags.c), lax.rem(i, lags.e)

        @pl.when(i >= lags.e)
        def _():
            for copy in second(i - lags.e, False):
                copy.wait_send()

        ey[e, :PART] = total(s_ref[s, 0, x, 1 - y, c], a2_ref[a, 0, x, 1 - y], cx[k, 1 - y, :PART]).astype(BF)
        ey[e, PART:] = total(s_ref[s, 2, x, 1 - y, c, :HALF], a2_ref[a, 2, x, 1 - y, :HALF], cx[k, 1 - y, PART:]).astype(BF)
        ex[e, :PART] = total(s_ref[s, 1, 1 - x, y, c], a2_ref[a, 1, 1 - x, y], cy[k, 1 - x, :PART]).astype(BF)
        ex[e, PART:] = total(s_ref[s, 2, 1 - x, y, c, HALF:], a2_ref[a, 2, 1 - x, y, HALF:], cy[k, 1 - x, PART:]).astype(BF)
        each(i, second, start)

    def take_third(i):
        each(i, second, lambda copy: copy.wait_recv())
        s, a, k, d, o = (lax.rem(i, n) for n in (lags.s, lags.a, lags.c, lags.d, 2))

        @pl.when(i >= 2)
        def _():
            for copy in outs(i - 2, False):
                copy.wait()

        gate = total(s_ref[s, 0, x, y, c], a2_ref[a, 0, x, y], cx[k, y, :PART], dy2[d, :PART]).astype(BF)
        up = total(s_ref[s, 1, x, y, c], a2_ref[a, 1, x, y], cy[k, x, :PART], dx[d, :PART]).astype(BF)
        og[o] = gate
        ou[o] = up
        low = total(s_ref[s, 2, x, y, c, :HALF], a2_ref[a, 2, x, y, :HALF], cx[k, y, PART:], dy2[d, PART:]).astype(BF)
        high = total(s_ref[s, 2, x, y, c, HALF:], a2_ref[a, 2, x, y, HALF:], cy[k, x, PART:], dx[d, PART:]).astype(BF)
        downs = [half[SUB * n : SUB * n + SUB] for half in (low, high) for n in range(HALF // SUB)]

        def squares(t):
            wide = t.astype(F32)
            return jnp.sum((wide * wide).reshape(-1, 8, t.shape[-1]), 0)

        @pl.when(i < STEPS - 1)
        def _():
            for n, one in enumerate(downs):
                od[o, :, BLOCK * n : BLOCK * n + BLOCK] = one
            sq_ref[...] += squares(gate) + squares(up) + squares(low) + squares(high)

        @pl.when(i == STEPS - 1)
        def _():
            for n, one in enumerate(downs):
                od[o, :LAST_SUB, BLOCK * n : BLOCK * n + LAST] = one[:LAST_SUB, :LAST]
                od[o, :LAST_SUB, BLOCK * n + LAST : BLOCK * n + BLOCK] = one[LAST_SUB:, :LAST]
            sq_ref[:, :LAST] += sum(squares(t[:, :LAST]) for t in (gate, up, low, high))

        each(i, outs, start)

    take_a = pltpu.make_async_copy(a_in, a_ref, a_sem.at[0])

    barrier = pltpu.get_barrier_semaphore()
    greeted = (to_core, to_x, to_y) if with_da else others

    @pl.when(j == 0)
    def _():
        take_a.start()
        for to in greeted:
            pl.semaphore_signal(barrier, inc=1, device_id=to, device_id_type=MESH)
        sq_ref[...] = jnp.zeros_like(sq_ref)
        if with_da:
            weights.start(j)

            @pl.loop(0, TOKENS // 256)
            def _(i):
                acc_ref[pl.ds(pl.multiple_of(i * 256, 256), 256), :] = jnp.zeros((256, D), F32)

    @pl.when(j < STEPS)
    def _():
        if with_da:
            weights.start(j + 1)
        s = lax.rem(j, lags.s)
        for i in range(4):
            r = slice(512 * i, 512 * i + 512)
            dh = dot(dy_ref[r, :], wd_ref[0], 1, 1).astype(BF).astype(F32)
            dgu_ref[r, :BLOCK] = (dh * q_ref[r, :]).astype(BF)
            dgu_ref[r, BLOCK:] = (dh * sl_ref[r, :]).astype(BF)

        pl.when(j == 0)(lambda: take_a.wait())

        @pl.when(j == STEPS - 1)
        def _():
            dgu_ref[:, LAST:BLOCK] = jnp.zeros((TOKENS, BLOCK - LAST), BF)
            dgu_ref[:, BLOCK + LAST :] = jnp.zeros((TOKENS, BLOCK - LAST), BF)

        for h in range(2):
            gu = dot(a_ref[:, D // 2 * h : D // 2 * (h + 1)], dgu_ref[...], 0, 0)
            for o in range(4):
                for t in range(2):
                    s_ref[s, t, h, o // 2, o % 2] = gu[PART * o : PART * o + PART, BLOCK * t : BLOCK * t + BLOCK].astype(BF)
        pl.when(j == 0)(lambda: pl.semaphore_wait(barrier, len(greeted)))
        each(j, functools.partial(pair, which=(0,)), start)
        for h in range(2):
            down = dot(ht_ref[...].reshape(BLOCK, TOKENS), dy_ref[:, D // 2 * h : D // 2 * (h + 1)], 1, 0)
            for o in range(8):
                for n in range(3):
                    s_ref[s, 2, o // 4, o // 2 % 2, o % 2, SUB * (3 * h + n) : SUB * (3 * h + n + 1)] = down[
                        SUB * o : SUB * o + SUB, BLOCK * n : BLOCK * n + BLOCK
                    ].astype(BF)

        @pl.when(j == STEPS - 1)
        def _():
            for o in range(8):
                for n in range(6):
                    at = o // 4, o // 2 % 2, o % 2
                    s_ref[(s, 2, *at, slice(SUB * n + LAST_SUB, SUB * n + SUB), slice(0, LAST))] = s_ref[
                        (s, 2, *at, slice(SUB * n, SUB * n + LAST_SUB), slice(LAST, BLOCK))
                    ]

        each(j, functools.partial(pair, which=(1,)), start)
        if with_da:
            weights.wait(j)
            for i in range(4):
                r = slice(512 * i, 512 * i + 512)
                acc_ref[r, :] += dot(dgu_ref[r, :], gu_ref[lax.rem(j, 2)], 1, 1)

    if with_da:
        take_h = pltpu.make_async_copy(h_in, a_ref, a_sem.at[1])
        give_dh = pltpu.make_async_copy(a_ref, dh_out, a_sem.at[2])
        pl.when(j == STEPS - 1)(lambda: take_h.start())

        @pl.when(j == STEPS)
        def _():
            take_h.wait()

            @pl.loop(0, TOKENS // 128)
            def _(i):
                r = pl.ds(pl.multiple_of(i * 128, 128), 128)
                h = a_ref[r, :].astype(F32)
                da = acc_ref[r, :].astype(BF).astype(F32)
                scale = lax.rsqrt(jnp.mean(h * h, -1, keepdims=True) + 1e-6)
                along = jnp.sum(da * h, -1, keepdims=True) * (scale * scale * scale) * (1.0 / D)
                a_ref[r, :] = dy_ref[r, :] + (da * scale - h * along).astype(BF)

            give_dh.start()

    pl.when((j >= lags.third) & (j < STEPS + lags.third))(lambda: take_third(j - lags.third))
    pl.when((j >= lags.second) & (j < STEPS + lags.second))(lambda: take_second(j - lags.second))
    pl.when(j < STEPS)(lambda: take_first(j))

    @pl.when(j == STEPS + lags.third - 1)
    def _():
        if not with_da:
            both = sq_ref[...] + other_ref[...]
            every_ref[me] = both[:, :128] + both[:, 128:]
            for n, to in enumerate(others):
                remote(every_ref.at[me], every_ref.at[me], f_send.at[n], f_recv.at[n], to).start()
        for i in range(STEPS - lags.b, STEPS):
            for copy in first(jnp.int32(i), i == STEPS - 1):
                copy.wait_send()
        for i in range(STEPS - lags.e, STEPS):
            for copy in second(jnp.int32(i), i == STEPS - 1):
                copy.wait_send()
        for i in range(STEPS - 2, STEPS):
            for copy in outs(jnp.int32(i), i == STEPS - 1):
                copy.wait()
        if with_da:
            give_dh.wait()
        else:
            for n, to in enumerate(others):
                remote(every_ref.at[me], every_ref.at[me], f_send.at[n], f_recv.at[n], to).wait()
            squares = functools.reduce(lambda p, q: p + q, [every_ref[n] for n in range(8)])
            squares = jnp.sum(jnp.sum(squares, axis=1, keepdims=True), axis=0, keepdims=True)
            f_ref[...] = jnp.broadcast_to(jnp.minimum(1.0, 0.5 * lax.rsqrt(squares / COUNT + 1e-30)), (8, 128))


def backward(l, lags, a, dy, wd, sl, q, ht, *more):
    with_da = l == 1
    at = lambda j: jnp.minimum(j, STEPS - 1)
    wide = pl.BlockSpec((TOKENS, BLOCK), lambda j: (0, at(j)))
    sums = pl.BlockSpec((8, BLOCK), lambda j: (0, 0))
    in_specs = [
        ANY,
        resident((TOKENS, D)),
        pl.BlockSpec((1, BLOCK, D), lambda j: (l, at(j), 0)),
        wide,
        wide,
        pl.BlockSpec((8, SUB, TOKENS), lambda j: (0, at(j), 0)),
    ]
    args = [a, dy, wd, sl, q, ht.reshape(8, OWN_DOWN, TOKENS), *more]
    out_shape = [jax.ShapeDtypeStruct((PART, FF), BF)] * 2 + [jax.ShapeDtypeStruct((OWN_DOWN, D), BF)]
    if with_da:
        in_specs += [ANY] * 3
        out_shape += [jax.ShapeDtypeStruct((8, BLOCK), F32), jax.ShapeDtypeStruct((TOKENS, D), BF)]
        out_specs = [ANY] * 3 + [sums, ANY]
        scratch = [pltpu.VMEM((TOKENS, D), F32), pltpu.VMEM((2, D, 2 * BLOCK), BF), pltpu.SemaphoreType.DMA((2, 3))]
    else:
        in_specs += [sums]
        out_shape += [jax.ShapeDtypeStruct((8, 128), F32)]
        out_specs = [ANY] * 3 + [pl.BlockSpec((8, 128), lambda j: (0, 0))]
        scratch = [pltpu.VMEM((8, BLOCK), F32), pltpu.VMEM((8, 8, 128), F32), *[pltpu.SemaphoreType.DMA((7,))] * 2]
    piece = (PART, BLOCK)
    scratch += [
        pltpu.VMEM((TOKENS, D), BF),
        pltpu.VMEM((TOKENS, 2 * BLOCK), BF),
        pltpu.VMEM((lags.s, 3, 2, 2, 2) + piece, BF),
        pltpu.VMEM((lags.a, 3, 2, 2) + piece, BF),
        *[pltpu.VMEM((lags.b, 2, CHUNK, BLOCK), BF)] * 2,
        *[pltpu.VMEM((lags.c, 2, CHUNK, BLOCK), BF)] * 2,
        *[pltpu.VMEM((lags.e, CHUNK, BLOCK), BF)] * 2,
        *[pltpu.VMEM((lags.d, CHUNK, BLOCK), BF)] * 2,
        *[pltpu.VMEM((2,) + piece, BF)] * 2,
        pltpu.VMEM((2, SUB, D), BF),
    ]
    scratch += [pltpu.SemaphoreType.DMA((n, 2)) for n in (lags.s, lags.a)]
    scratch += [pltpu.SemaphoreType.DMA((n,)) for n in (lags.b, lags.b, lags.c, lags.c, lags.e, lags.e, lags.d, lags.d)]
    scratch += [pltpu.SemaphoreType.DMA((2, 3)), pltpu.SemaphoreType.DMA((3,))]
    return pl.pallas_call(
        functools.partial(backward_kernel, l, lags),
        grid=(STEPS + lags.third,),
        in_specs=in_specs,
        out_specs=out_specs,
        out_shape=out_shape,
        scratch_shapes=scratch,
        compiler_params=pltpu.CompilerParams(vmem_limit_bytes=VMEM_LIMIT, collective_id=l, has_side_effects=True),
        cost_estimate=cost(6 if with_da else 4, 150e6),
    )(*args)


def adamw_kernel(at_ref, f_ref, g_ref, w_ref, m_ref, v_ref, *refs):
    nw_ref, nm_ref, nv_ref = refs[-3:]
    factor = f_ref[0:1, 0:1]

    @pl.loop(0, g_ref.shape[0] // 16)
    def _(i):
        r = pl.ds(pl.multiple_of(i * 16, 16), 16)
        g = g_ref[r, :].astype(F32) * factor
        w = w_ref[0, r, :].astype(F32)
        m = 0.9 * m_ref[0, r, :] + 0.1 * g
        v = 0.95 * v_ref[0, r, :] + 0.05 * g * g
        nm_ref[0, r, :] = m
        nv_ref[0, r, :] = v
        nw_ref[r, :] = (w - 0.02 * (m * lax.rsqrt(v + 1e-8) + 0.1 * w)).astype(BF)


def adamw(l, skip, count, at, factor, g, w, m, v, so_far=None):
    rows, columns = g.shape
    deep = rows // 3
    moment = pl.BlockSpec((1, deep, columns), lambda i, at: (l, skip + i, 0))
    in_specs = [
        pl.BlockSpec((8, 128), lambda i, at: (0, 0)),
        pl.BlockSpec((deep, columns), lambda i, at: (skip + i, 0)),
        pl.BlockSpec((1, deep, columns), lambda i, at: (l, 3 * at[0] + skip + i, 0)),
        moment,
        moment,
    ]
    args = [factor, g, w, m, v]
    aliases = {}
    if so_far is not None:
        in_specs += [ANY, ANY]
        args += so_far
        aliases = {6: 1, 7: 2}
    return pl.pallas_call(
        adamw_kernel,
        grid_spec=pltpu.PrefetchScalarGridSpec(
            num_scalar_prefetch=1,
            grid=(count,),
            in_specs=in_specs,
            out_specs=[pl.BlockSpec((deep, columns), lambda i, at: (i, 0)), moment, moment],
        ),
        out_shape=[jax.ShapeDtypeStruct((count * deep, columns), BF)] + [jax.ShapeDtypeStruct(m.shape, F32)] * 2,
        input_output_aliases=aliases,
        compiler_params=pltpu.CompilerParams(vmem_limit_bytes=48 << 20),
        cost_estimate=cost(0.03 * count, 22 * count * deep * columns),
    )(at, *args)


def place_kernel(n, owners_ref, *refs):
    out_ref = refs[-1]
    s = pl.program_id(0)
    for k in range(n):

        @pl.when(s == k)
        def _():
            out_ref[0] = refs[k][...]


def place(l, skip, count, owners, pieces, so_far, whole):
    n = len(pieces)
    rows, columns = pieces[0].shape
    deep = rows // count

    def of(k):
        return lambda s, i, own: (jnp.where(s == k, i, jnp.where(s < k, 0, count - 1)), 0)

    in_specs = [pl.BlockSpec((deep, columns), of(k)) for k in range(n)]
    args = list(pieces)
    aliases = {}
    if so_far is not None:
        in_specs.append(ANY)
        args.append(so_far)
        aliases = {n + 1: 0}
    return pl.pallas_call(
        functools.partial(place_kernel, n),
        grid_spec=pltpu.PrefetchScalarGridSpec(
            num_scalar_prefetch=1,
            grid=(n, count),
            in_specs=in_specs,
            out_specs=pl.BlockSpec((1, deep, columns), lambda s, i, own: (l, 3 * own[s] + skip + i, 0)),
        ),
        out_shape=jax.ShapeDtypeStruct(whole.shape, BF),
        input_output_aliases=aliases,
        compiler_params=pltpu.CompilerParams(vmem_limit_bytes=48 << 20),
        cost_estimate=cost(0.03 * n * count, 4 * n * rows * columns),
    )(owners, *args)


PIECES = [(0, l, 0, 1) for l in range(2)] + [(0, l, 1, 2) for l in range(2)] + [(1, l, 0, 3) for l in range(2)]
PIECES += [(2, l, 0, 2) for l in range(2)] + [(2, l, 2, 1) for l in range(2)]


def solution(mesh):
    def swap(t, mask):
        return lax.ppermute(t, "dp", [(i, i ^ mask) for i in range(8)])

    def step(x, dy, wg, wu, wd, mg, mu, md, vg, vu, vd):
        x, dy = x[0], dy[0]
        me = lax.axis_index("dp")
        a0, ht0, sl0, q0, h1 = forward(0, x, wg, wu, wd)
        a1, ht1, sl1, q1 = forward(1, h1, wg, wu)
        *g1, squares, dh1 = backward(1, Lags(1, 2, 2, 2), a1, dy, wd, sl1, q1, ht1, wg, wu, h1)
        *g0, factor = backward(0, Lags(2, 4, 3, 3), a0, dh1, wd, sl0, q0, ht0, squares)
        at = me[None].astype(jnp.int32)
        groups = {name: jnp.stack([me ^ k for k in group]).astype(jnp.int32) for name, group in GROUPS.items()}
        mats = ((wg, mg, vg), (wu, mu, vu), (wd, md, vd))
        moments, whole = [None] * 3, [None] * 3

        def put(kind, number, have):
            n, l, skip, count = PIECES[number]
            whole[n] = place(l, skip, count, groups[kind], [have[k] for k in GROUPS[kind]], whole[n], mats[n][0])

        everything = []
        for number, (n, l, skip, count) in enumerate(PIECES):
            have = {}
            everything.append(have)
            have[0], *moments[n] = adamw(l, skip, count, at, factor, (g0, g1)[l][n], *mats[n], moments[n])
            have[4] = swap(have[0], 4)
            have[2] = swap(have[0], 2)
            have[6] = swap(have[4], 2) if number % 2 else swap(have[2], 4)
            for k in (0, 4, 2, 6):
                have[k + 1] = swap(have[k], 1)
            put("own", number, have)
            put("near", number, have)
        for number, have in enumerate(everything):
            put("across", number, have)
            put("last", number, have)
        return tuple(whole + [m[0] for m in moments] + [m[1] for m in moments])

    whole, rows = P(None, None, None), P(None, "dp", None)
    return jax.shard_map(
        step,
        mesh=mesh,
        in_specs=(P(("rep", "dp")),) * 2 + (whole,) * 3 + (rows,) * 6,
        out_specs=(P("rep"),) * 3 + (P("rep", "dp"),) * 6,
        check_vma=False,
    )
```

```python
import functools

import jax
import jax.numpy as jnp
from jax import lax
from jax.experimental import pallas as pl
from jax.experimental.pallas import tpu as pltpu
from jax.sharding import PartitionSpec as P


BF = jnp.bfloat16
F32 = jnp.float32
MESH = pl.DeviceIdType.MESH
TOKENS, D, FF, LAYERS = 2048, 1536, 4224, 2
BLOCK = 256
STEPS = -(-FF // BLOCK)
LAST = FF - (STEPS - 1) * BLOCK
PART = D // 8
SUB = BLOCK // 8
OWN_DOWN = FF // 8
LAST_SUB = OWN_DOWN - (STEPS - 1) * SUB
HALF = PART // 2
CHUNK = PART + HALF
COUNT = 3 * LAYERS * D * FF
THIRD = FF // 3
GATE, UP, DOWN = range(3)
AHEAD = 2 * THIRD
TILES = AHEAD // BLOCK
SPREAD = 13
VMEM_LIMIT = 67043328
SMALL_LIMIT = 48 << 20


ANY = pl.BlockSpec(memory_space=pl.ANY)
SQUEEZED = pl.Squeezed()
FACTOR = (8, 128)
FIRST = pl.BlockSpec(FACTOR, lambda *_: (0, 0))
GROUPS = {"own": (0, 1), "near": (4, 2, 5, 3), "across": (6,), "last": (7,), "ahead_own": (4, 2, 6), "ahead_partner": (5, 3, 7)}


def dot(a, b, dims="nn"):
    ca, cb = ("tn".index(dims[0]), "nt".index(dims[1]))
    return lax.dot_general(a, b, (((ca,), (cb,)), ((), ())), preferred_element_type=F32)


def resident(shape):
    return pl.BlockSpec(shape, lambda *_: (0,) * len(shape), pipeline_mode=pl.Buffered(1))


def cost(units, bytes_accessed):
    return pl.CostEstimate(flops=int(units * 2 * TOKENS * D * FF), bytes_accessed=int(bytes_accessed), transcendentals=0)


def normed(h):
    wide = h.astype(F32)
    scale = lax.rsqrt(jnp.mean(wide * wide, -1, keepdims=True) + 1e-6)
    return (wide * scale).astype(BF)


def neighbours():
    me = lax.axis_index("dp")
    x, y, c = lax.div(me, 4), lax.rem(lax.div(me, 2), 2), lax.rem(me, 2)
    return (me, x, y, c), [{"dp": me + k * (1 - 2 * t)} for k, t in ((1, c), (4, x), (2, y))]


def remote(src, dst, send, recv, to):
    return pltpu.make_async_remote_copy(src_ref=src, dst_ref=dst, send_sem=send, recv_sem=recv, device_id=to, device_id_type=MESH)


class Weights:
    def __init__(self, l, wg, wu, wd, gu_ref, down_ref, sems):
        self.l, self.wg, self.wu, self.wd, self.gu_ref, self.down_ref, self.sems = l, wg, wu, wd, gu_ref, down_ref, sems

    def copies(self, j, last):
        slot, block, l = lax.rem(j, 2), lax.rem(j, STEPS), self.l
        if l is None:
            l = lax.div(j, STEPS)
        width = LAST if last else BLOCK
        start = (STEPS - 1) * BLOCK if last else pl.multiple_of(block * BLOCK, BLOCK)
        columns = pl.ds(start, width)
        pairs = [
            (self.wg.at[l, :, columns], self.gu_ref.at[slot, :, pl.ds(0, width)]),
            (self.wu.at[l, :, columns], self.gu_ref.at[slot, :, pl.ds(BLOCK, width)]),
        ]
        if self.wd is not None:
            pairs.append((self.wd.at[l, columns], self.down_ref.at[slot, pl.ds(0, width)]))
        return [pltpu.make_async_copy(src, dst, self.sems.at[slot, n]) for n, (src, dst) in enumerate(pairs)]

    def each(self, j, act):
        block = lax.rem(j, STEPS)

        @pl.when(block < STEPS - 1)
        def _():
            for copy in self.copies(j, False):
                act(copy)

        @pl.when(block == STEPS - 1)
        def _():
            for copy in self.copies(j, True):
                act(copy)

    def start(self, j):
        self.each(j, lambda copy: copy.start())

    def wait(self, j):
        self.each(j, lambda copy: copy.wait())


def forward_kernel(x_ref, wg, wu, wd, m_in, v_in, *refs):
    a_out, ht_ref, sl_ref, q_ref, h_out, mv_out, *refs = refs
    a_ref, h_ref, gu_ref, down_ref, hid_ref, acc_ref, w_sems, sems, near_send, near_recv, far_send, far_recv = refs
    j = pl.program_id(0)
    block = lax.rem(j, STEPS)
    weights = Weights(None, wg, wu, wd, gu_ref, down_ref, w_sems)
    _, (_, to_x, to_y) = neighbours()
    barrier = pltpu.get_barrier_semaphore()
    keep = [pltpu.make_async_copy(a_ref, a_out.at[l], sems.at[l]) for l in range(LAYERS)]
    keep_h = pltpu.make_async_copy(h_ref, h_out, sems.at[2])

    def near(k):
        src = (m_in, v_in)[k].at[1, :, pl.ds(0, AHEAD)]
        return [remote(src, mv_out.at[k, n], near_send.at[k, n], near_recv.at[k, n], to) for n, to in enumerate((to_x, to_y))]

    def far(k):
        return [
            remote(mv_out.at[k, n, rows], mv_out.at[k, 2, rows], far_send.at[k, n], far_recv.at[k, n], to)
            for n, (rows, to) in enumerate(((pl.ds(0, HALF), to_y), (pl.ds(HALF, HALF), to_x)))
        ]

    @pl.when(j == 0)
    def _():
        for to in (to_x, to_y):
            pl.semaphore_signal(barrier, inc=1, device_id=to, device_id_type=MESH)
        weights.start(j)

        @pl.loop(0, TOKENS // 256)
        def _(i):
            r = pl.ds(pl.multiple_of(i * 256, 256), 256)
            a_ref[r, :] = normed(x_ref[r, :])
            acc_ref[r, :] = jnp.zeros((256, D), F32)

        keep[0].start()

    @pl.when(j == 2)
    def _():
        pl.semaphore_wait(barrier, 2)
        for k in range(2):
            for copy in near(k):
                copy.start()

    @pl.when(j == STEPS)
    def _():
        keep[0].wait()

        @pl.loop(0, TOKENS // 256)
        def _(i):
            r = pl.ds(pl.multiple_of(i * 256, 256), 256)
            h = x_ref[r, :] + acc_ref[r, :].astype(BF)
            h_ref[r, :] = h
            a_ref[r, :] = normed(h)

        keep[1].start()
        keep_h.start()

    @pl.when(j == STEPS + 4)
    def _():
        for k in range(2):
            for copy in near(k):
                copy.wait()
            for copy in far(k):
                copy.start()

    pl.when(j + 1 < LAYERS * STEPS)(lambda: weights.start(j + 1))
    weights.wait(j)
    slot = lax.rem(j, 2)
    for i in range(8):
        r = slice(256 * i, 256 * i + 256)
        gu = dot(a_ref[r, :], gu_ref[slot])
        g, u = gu[:, :BLOCK], gu[:, BLOCK:]
        s = jax.nn.sigmoid(g)
        sl = g * s
        sl_ref[0, r, :] = sl
        q_ref[0, r, :] = u * (s * (1.0 + g * (1.0 - s)))
        hid = (sl * u).astype(BF)
        hid_ref[r, :] = hid
        ht_ref[0, :, r] = hid.T

    @pl.when(j < STEPS)
    def _():
        @pl.when(block == STEPS - 1)
        def _():
            hid_ref[:, LAST:] = jnp.zeros((TOKENS, BLOCK - LAST), BF)

        acc_ref[...] += dot(hid_ref[...], down_ref[slot])

    @pl.when(j == LAYERS * STEPS - 1)
    def _():
        keep[1].wait()
        keep_h.wait()
        for k in range(2):
            for copy in far(k):
                copy.wait()


def forward(x, wg, wu, wd, m, v):
    layer = lambda j: lax.div(j, STEPS)
    block = lambda j: lax.rem(j, STEPS)
    wide = pl.BlockSpec((1, TOKENS, BLOCK), lambda j: (layer(j), 0, block(j)))
    shape = jax.ShapeDtypeStruct
    return pl.pallas_call(
        forward_kernel,
        grid=(LAYERS * STEPS,),
        in_specs=[resident((TOKENS, D))] + [ANY] * 5,
        out_specs=[ANY, pl.BlockSpec((1, BLOCK, TOKENS), lambda j: (layer(j), block(j), 0)), wide, wide, ANY, ANY],
        out_shape=[
            shape((LAYERS, TOKENS, D), BF),
            shape((LAYERS, FF, TOKENS), BF),
            *[shape((LAYERS, TOKENS, FF), F32)] * 2,
            shape((TOKENS, D), BF),
            shape((2, 3, PART, AHEAD), F32),
        ],
        scratch_shapes=[
            pltpu.VMEM((TOKENS, D), BF),
            pltpu.VMEM((TOKENS, D), BF),
            pltpu.VMEM((2, D, 2 * BLOCK), BF),
            pltpu.VMEM((2, BLOCK, D), BF),
            pltpu.VMEM((TOKENS, BLOCK), BF),
            pltpu.VMEM((TOKENS, D), F32),
            pltpu.SemaphoreType.DMA((2, 3)),
            pltpu.SemaphoreType.DMA((3,)),
            *[pltpu.SemaphoreType.DMA((2, 2))] * 4,
        ],
        compiler_params=pltpu.CompilerParams(vmem_limit_bytes=VMEM_LIMIT, collective_id=2, has_side_effects=True),
        cost_estimate=cost(5, 260e6),
        name="forward",
    )(x, wg, wu, wd, m, v)


def bits(o):
    return o // 4, o // 2 % 2, o % 2


class Lags:
    def __init__(self, second, third, b, e):
        self.second, self.third, self.b, self.e = second, third, b, e
        self.s = third + 1
        self.a = third + 2
        self.c = second + third
        self.d = 2 * (third - second)


def backward_kernel(l, lags, a_in, dy_ref, wd_ref, sl_ref, q_ref, ht_ref, *refs):
    with_da = l == 1
    if with_da:
        wg, wu, h_in, g_gate, g_up, g_down, sq_ref, dh_out, far_out, acc_ref, gu_ref, w_sems, *refs = refs
        near_send, near_recv, far_send, far_recv, *refs = refs
        weights = Weights(l, wg, wu, None, gu_ref, None, w_sems)
    else:
        other_ref, g_gate, g_up, g_down, f_ref, sq_ref, every_ref, f_send, f_recv, *refs = refs
    a_ref, dgu_ref, s_ref, a2_ref, bx, by, cx, cy, ex, ey, dx, dy2, og, ou, od, *sems = refs
    s_send, a_recv, bx_send, by_send, cx_recv, cy_recv, ex_send, ey_send, dx_recv, dy_recv, out_sem, a_sem = sems
    j = pl.program_id(0)
    (me, x, y, c), (to_core, to_x, to_y) = neighbours()
    xn, yn, cn = (1 - k for k in (x, y, c))
    others = [{"dp": lax.rem(me + k, 8)} for k in range(1, 8)]

    def columns(last):
        return pl.ds(0, LAST if last else BLOCK)

    def pair(i, last, which=(0, 1)):
        s, a, w = lax.rem(i, lags.s), lax.rem(i, lags.a), columns(last)
        return [
            remote(s_ref.at[s, n, :, :, cn, :, w], a2_ref.at[a, n, :, :, :, w], s_send.at[s, k], a_recv.at[a, k], to_core)
            for k, n in ((k, (pl.ds(0, 2), pl.ds(2, 1))[k]) for k in which)
        ]

    def first(i, last):
        b, k, w = lax.rem(i, lags.b), lax.rem(i, lags.c), columns(last)
        return [
            remote(bx.at[b, :, :, w], cx.at[k, :, :, w], bx_send.at[b], cx_recv.at[k], to_x),
            remote(by.at[b, :, :, w], cy.at[k, :, :, w], by_send.at[b], cy_recv.at[k], to_y),
        ]

    def second(i, last):
        e, k, w = lax.rem(i, lags.e), lax.rem(i, lags.d), columns(last)
        return [
            remote(ex.at[e, :, w], dx.at[k, :, w], ex_send.at[e], dx_recv.at[k], to_x),
            remote(ey.at[e, :, w], dy2.at[k, :, w], ey_send.at[e], dy_recv.at[k], to_y),
        ]

    def outs(i, last):
        o, p = lax.rem(i, 2), lax.rem(i, og.shape[0])
        if last:
            wide, deep = pl.ds((STEPS - 1) * BLOCK, LAST), pl.ds((STEPS - 1) * SUB, LAST_SUB)
            srcs = og.at[p, :, pl.ds(0, LAST)], ou.at[o, :, pl.ds(0, LAST)], od.at[o, pl.ds(0, LAST_SUB)]
        else:
            wide, deep = pl.ds(pl.multiple_of(i * BLOCK, BLOCK), BLOCK), pl.ds(pl.multiple_of(i * SUB, SUB), SUB)
            srcs = og.at[p], ou.at[o], od.at[o]
        dsts = g_gate.at[:, wide], g_up.at[:, wide], g_down.at[deep]
        return [pltpu.make_async_copy(s, d, out_sem.at[o, n]) for n, (s, d) in enumerate(zip(srcs, dsts))]

    def each(i, copies, act):
        @pl.when(i < STEPS - 1)
        def _():
            for copy in copies(i, False):
                act(copy)

        @pl.when(i == STEPS - 1)
        def _():
            for copy in copies(i, True):
                act(copy)

    def start(copy):
        copy.start()

    def total(*terms):
        return functools.reduce(lambda p, q: p + q, [t.astype(F32) for t in terms])

    def take_first(i):
        each(i, pair, lambda copy: copy.wait())
        s, a, b = lax.rem(i, lags.s), lax.rem(i, lags.a), lax.rem(i, lags.b)

        @pl.when(i >= lags.b)
        def _():
            for copy in first(i - lags.b, False):
                copy.wait_send()

        for t in range(2):
            bx[b, t, :PART] = total(s_ref[s, GATE, xn, t, c], a2_ref[a, GATE, xn, t]).astype(BF)
            bx[b, t, PART:] = total(s_ref[s, DOWN, xn, t, c, :HALF], a2_ref[a, DOWN, xn, t, :HALF]).astype(BF)
            by[b, t, :PART] = total(s_ref[s, UP, t, yn, c], a2_ref[a, UP, t, yn]).astype(BF)
            by[b, t, PART:] = total(s_ref[s, DOWN, t, yn, c, HALF:], a2_ref[a, DOWN, t, yn, HALF:]).astype(BF)
        each(i, first, start)

    def take_second(i):
        each(i, first, lambda copy: copy.wait_recv())
        s, a, k, e = lax.rem(i, lags.s), lax.rem(i, lags.a), lax.rem(i, lags.c), lax.rem(i, lags.e)

        @pl.when(i >= lags.e)
        def _():
            for copy in second(i - lags.e, False):
                copy.wait_send()

        ey[e, :PART] = total(s_ref[s, GATE, x, yn, c], a2_ref[a, GATE, x, yn], cx[k, yn, :PART]).astype(BF)
        ey[e, PART:] = total(s_ref[s, DOWN, x, yn, c, :HALF], a2_ref[a, DOWN, x, yn, :HALF], cx[k, yn, PART:]).astype(BF)
        ex[e, :PART] = total(s_ref[s, UP, xn, y, c], a2_ref[a, UP, xn, y], cy[k, xn, :PART]).astype(BF)
        ex[e, PART:] = total(s_ref[s, DOWN, xn, y, c, HALF:], a2_ref[a, DOWN, xn, y, HALF:], cy[k, xn, PART:]).astype(BF)
        each(i, second, start)

    def take_third(i):
        each(i, second, lambda copy: copy.wait_recv())
        s, a, k, d, o = (lax.rem(i, n) for n in (lags.s, lags.a, lags.c, lags.d, 2))

        @pl.when(i >= 1)
        def _():
            for copy in outs(i - 1, False):
                copy.wait()

        gate = total(s_ref[s, GATE, x, y, c], a2_ref[a, GATE, x, y], cx[k, y, :PART], dy2[d, :PART]).astype(BF)
        up = total(s_ref[s, UP, x, y, c], a2_ref[a, UP, x, y], cy[k, x, :PART], dx[d, :PART]).astype(BF)
        og[lax.rem(i, og.shape[0])] = gate
        ou[o] = up
        low = total(s_ref[s, DOWN, x, y, c, :HALF], a2_ref[a, DOWN, x, y, :HALF], cx[k, y, PART:], dy2[d, PART:]).astype(BF)
        high = total(s_ref[s, DOWN, x, y, c, HALF:], a2_ref[a, DOWN, x, y, HALF:], cy[k, x, PART:], dx[d, PART:]).astype(BF)
        downs = [half[SUB * n : SUB * n + SUB] for half in (low, high) for n in range(HALF // SUB)]

        def squares(t):
            wide = t.astype(F32)
            return jnp.sum((wide * wide).reshape(-1, 8, t.shape[-1]), 0)

        @pl.when(i < STEPS - 1)
        def _():
            for n, one in enumerate(downs):
                od[o, :, BLOCK * n : BLOCK * n + BLOCK] = one
            sq_ref[...] += squares(gate) + squares(up) + squares(low) + squares(high)

        @pl.when(i == STEPS - 1)
        def _():
            for n, one in enumerate(downs):
                od[o, :LAST_SUB, BLOCK * n : BLOCK * n + LAST] = one[:LAST_SUB, :LAST]
                od[o, :LAST_SUB, BLOCK * n + LAST : BLOCK * n + BLOCK] = one[LAST_SUB:, :LAST]
            sq_ref[:, :LAST] += sum(squares(t[:, :LAST]) for t in (gate, up, low, high))

        each(i, outs, start)

    def near(t):
        k = lax.rem(t, 4)
        src = og.at[lax.rem(t, og.shape[0])]
        return [remote(src, far_out.at[n, t], near_send.at[k, n], near_recv.at[k, n], to) for n, to in enumerate((to_x, to_y))]

    def far(t):
        k = lax.rem(t, 4)
        return [
            remote(far_out.at[n, t, rows], far_out.at[2, t, rows], far_send.at[k, n], far_recv.at[k, n], to)
            for n, (rows, to) in enumerate(((pl.ds(0, HALF), to_y), (pl.ds(HALF, HALF), to_x)))
        ]

    def at_step(n, act):
        t = lax.div(n * TILES, SPREAD)

        @pl.when((n >= 0) & (n < SPREAD) & ((n == 0) | (t > lax.div((n - 1) * TILES, SPREAD))))
        def _():
            act(t)

    def pass_on(t):
        for copy in near(t):
            copy.wait()
        for copy in far(t):
            copy.start()

    take_a = pltpu.make_async_copy(a_in.at[l], a_ref, a_sem.at[0])

    barrier = pltpu.get_barrier_semaphore()
    greeted = (to_core, to_x, to_y) if with_da else others

    @pl.when(j == 0)
    def _():
        take_a.start()
        for to in greeted:
            pl.semaphore_signal(barrier, inc=1, device_id=to, device_id_type=MESH)
        sq_ref[...] = jnp.zeros_like(sq_ref)
        if with_da:
            weights.start(j)

            @pl.loop(0, TOKENS // 256)
            def _(i):
                acc_ref[pl.ds(pl.multiple_of(i * 256, 256), 256), :] = jnp.zeros((256, D), F32)

    @pl.when(j < STEPS)
    def _():
        if with_da:
            pl.when(j + 1 < STEPS)(lambda: weights.start(j + 1))
        s = lax.rem(j, lags.s)
        for i in range(4):
            r = slice(512 * i, 512 * i + 512)
            dh = dot(dy_ref[r, :], wd_ref[0], "nt").astype(BF).astype(F32)
            dgu_ref[r, :BLOCK] = (dh * q_ref[0, r, :]).astype(BF)
            dgu_ref[r, BLOCK:] = (dh * sl_ref[0, r, :]).astype(BF)

        pl.when(j == 0)(lambda: take_a.wait())

        @pl.when(j == STEPS - 1)
        def _():
            dgu_ref[:, LAST:BLOCK] = jnp.zeros((TOKENS, BLOCK - LAST), BF)
            dgu_ref[:, BLOCK + LAST :] = jnp.zeros((TOKENS, BLOCK - LAST), BF)

        for h in range(2):
            gu = dot(a_ref[:, D // 2 * h : D // 2 * (h + 1)], dgu_ref[...], "tn")
            for o in range(4):
                for t in range(2):
                    s_ref[s, t, h, o // 2, o % 2] = gu[PART * o : PART * o + PART, BLOCK * t : BLOCK * t + BLOCK].astype(BF)
        pl.when(j == 0)(lambda: pl.semaphore_wait(barrier, len(greeted)))
        each(j, functools.partial(pair, which=(0,)), start)
        for h in range(2):
            down = dot(ht_ref[...].reshape(BLOCK, TOKENS), dy_ref[:, D // 2 * h : D // 2 * (h + 1)])
            for o in range(8):
                for n in range(3):
                    s_ref[(s, DOWN, *bits(o), slice(SUB * (3 * h + n), SUB * (3 * h + n + 1)))] = down[
                        SUB * o : SUB * o + SUB, BLOCK * n : BLOCK * n + BLOCK
                    ].astype(BF)

        @pl.when(j == STEPS - 1)
        def _():
            for o in range(8):
                for n in range(6):
                    half = SUB * n + LAST_SUB
                    s_ref[(s, DOWN, *bits(o), slice(half, SUB * n + SUB), slice(LAST))] = s_ref[
                        (s, DOWN, *bits(o), slice(SUB * n, half), slice(LAST, BLOCK))
                    ]

        each(j, functools.partial(pair, which=(1,)), start)
        if with_da:
            weights.wait(j)
            for i in range(4):
                r = slice(512 * i, 512 * i + 512)
                acc_ref[r, :] += dot(dgu_ref[r, :], gu_ref[lax.rem(j, 2)], "nt")

    if with_da:
        take_h = pltpu.make_async_copy(h_in, a_ref, a_sem.at[1])
        give_dh = pltpu.make_async_copy(a_ref, dh_out, a_sem.at[2])
        pl.when(j == STEPS - 1)(lambda: take_h.start())

        @pl.when(j == STEPS)
        def _():
            take_h.wait()

            @pl.loop(0, TOKENS // 128)
            def _(i):
                r = pl.ds(pl.multiple_of(i * 128, 128), 128)
                h = a_ref[r, :].astype(F32)
                da = acc_ref[r, :].astype(BF).astype(F32)
                scale = lax.rsqrt(jnp.mean(h * h, -1, keepdims=True) + 1e-6)
                along = jnp.sum(da * h, -1, keepdims=True) * (scale * scale * scale) * (1.0 / D)
                a_ref[r, :] = dy_ref[r, :] + (da * scale - h * along).astype(BF)

            give_dh.start()

    pl.when((j >= lags.third) & (j < STEPS + lags.third))(lambda: take_third(j - lags.third))
    pl.when((j >= lags.second) & (j < STEPS + lags.second))(lambda: take_second(j - lags.second))
    pl.when(j < STEPS)(lambda: take_first(j))
    if with_da:
        soonest = lags.third
        at_step(j - soonest - 4, lambda t: [copy.wait() for copy in far(t)])
        at_step(j - soonest - 2, pass_on)
        at_step(j - soonest, lambda t: [copy.start() for copy in near(t)])

    @pl.when(j == STEPS + lags.third - 1)
    def _():
        if not with_da:
            both = sq_ref[...] + other_ref[...]
            every_ref[me] = both[:, :128] + both[:, 128:]
            for n, to in enumerate(others):
                remote(every_ref.at[me], every_ref.at[me], f_send.at[n], f_recv.at[n], to).start()
        for i in range(STEPS - lags.b, STEPS):
            for copy in first(jnp.int32(i), i == STEPS - 1):
                copy.wait_send()
        for i in range(STEPS - lags.e, STEPS):
            for copy in second(jnp.int32(i), i == STEPS - 1):
                copy.wait_send()
        for copy in outs(jnp.int32(STEPS - 1), True):
            copy.wait()
        if with_da:
            give_dh.wait()
        else:
            for n, to in enumerate(others):
                remote(every_ref.at[me], every_ref.at[me], f_send.at[n], f_recv.at[n], to).wait()
            squares = functools.reduce(lambda p, q: p + q, [every_ref[n] for n in range(8)])
            squares = jnp.sum(jnp.sum(squares, axis=1, keepdims=True), axis=0, keepdims=True)
            f_ref[...] = jnp.broadcast_to(jnp.minimum(1.0, 0.5 * lax.rsqrt(squares / COUNT + 1e-30)), FACTOR)


def backward(l, lags, a, dy, wd, sl, q, ht, *more):
    with_da = l == 1
    at = lambda j: jnp.minimum(j, STEPS - 1)
    wide = pl.BlockSpec((1, TOKENS, BLOCK), lambda j: (l, 0, at(j)))
    sums = pl.BlockSpec((8, BLOCK), lambda j: (0, 0))
    in_specs = [
        ANY,
        resident((TOKENS, D)),
        pl.BlockSpec((1, BLOCK, D), lambda j: (l, at(j), 0)),
        wide,
        wide,
        pl.BlockSpec((8, SUB, TOKENS), lambda j: (l, at(j), 0)),
    ]
    args = [a, dy, wd, sl, q, ht.reshape(LAYERS * 8, OWN_DOWN, TOKENS), *more]
    out_shape = [jax.ShapeDtypeStruct((PART, FF), BF)] * 2 + [jax.ShapeDtypeStruct((OWN_DOWN, D), BF)]
    if with_da:
        in_specs += [ANY] * 3
        out_shape += [jax.ShapeDtypeStruct(*t) for t in (((8, BLOCK), F32), ((TOKENS, D), BF), ((3, TILES) + (PART, BLOCK), BF))]
        out_specs = [ANY] * 3 + [sums, ANY, ANY]
        scratch = [pltpu.VMEM((TOKENS, D), F32), pltpu.VMEM((2, D, 2 * BLOCK), BF), pltpu.SemaphoreType.DMA((2, 3))]
        scratch += [pltpu.SemaphoreType.DMA((4, 2))] * 4
    else:
        in_specs += [sums]
        out_shape += [jax.ShapeDtypeStruct(FACTOR, F32)]
        out_specs = [ANY] * 3 + [FIRST]
        scratch = [pltpu.VMEM((8, BLOCK), F32), pltpu.VMEM((8, 8, 128), F32), *[pltpu.SemaphoreType.DMA((7,))] * 2]
    piece = (PART, BLOCK)
    scratch += [
        pltpu.VMEM((TOKENS, D), BF),
        pltpu.VMEM((TOKENS, 2 * BLOCK), BF),
        pltpu.VMEM((lags.s, 3, 2, 2, 2) + piece, BF),
        pltpu.VMEM((lags.a, 3, 2, 2) + piece, BF),
        *[pltpu.VMEM((lags.b, 2, CHUNK, BLOCK), BF)] * 2,
        *[pltpu.VMEM((lags.c, 2, CHUNK, BLOCK), BF)] * 2,
        *[pltpu.VMEM((lags.e, CHUNK, BLOCK), BF)] * 2,
        *[pltpu.VMEM((lags.d, CHUNK, BLOCK), BF)] * 2,
        pltpu.VMEM((6 if with_da else 2,) + piece, BF),
        pltpu.VMEM((2,) + piece, BF),
        pltpu.VMEM((2, SUB, D), BF),
    ]
    scratch += [pltpu.SemaphoreType.DMA((n, 2)) for n in (lags.s, lags.a)]
    scratch += [pltpu.SemaphoreType.DMA((n,)) for n in (lags.b, lags.b, lags.c, lags.c, lags.e, lags.e, lags.d, lags.d)]
    scratch += [pltpu.SemaphoreType.DMA((2, 3)), pltpu.SemaphoreType.DMA((3,))]
    return pl.pallas_call(
        functools.partial(backward_kernel, l, lags),
        grid=(STEPS + lags.third,),
        in_specs=in_specs,
        out_specs=out_specs,
        out_shape=out_shape,
        scratch_shapes=scratch,
        compiler_params=pltpu.CompilerParams(vmem_limit_bytes=VMEM_LIMIT, collective_id=l, has_side_effects=True),
        cost_estimate=cost(6 if with_da else 4, 150e6),
    )(*args)


def stepped(factor, g, w, m, v):
    g, w = g.astype(F32) * factor, w.astype(F32)
    m = 0.9 * m + 0.1 * g
    v = 0.95 * v + 0.05 * g * g
    return (w - 0.02 * (m * lax.rsqrt(v + 1e-8) + 0.1 * w)).astype(BF), m, v


def adamw_kernel(at_ref, f_ref, g_ref, w_ref, m_ref, v_ref, *refs):
    nw_ref, nm_ref, nv_ref = refs[-3:]
    factor = f_ref[:1, :1]

    @pl.loop(0, g_ref.shape[0] // 16)
    def _(i):
        r = pl.ds(pl.multiple_of(i * 16, 16), 16)
        nw_ref[r, :], nm_ref[0, r, :], nv_ref[0, r, :] = stepped(factor, g_ref[r, :], w_ref[0, r, :], m_ref[0, r, :], v_ref[0, r, :])


def thirds(shape, axis):
    return tuple(n // 3 if k == axis else n for k, n in enumerate(shape))


def spot(axis, i, other=0):
    return (i, other) if axis == 0 else (other, i)


def adamw(piece, at, factor, g, w, m, v, so_far=None):
    _, l, axis, skip, count = piece
    block = thirds(g.shape, axis)
    moment = pl.BlockSpec((1, *block), lambda i, at: (l, *spot(axis, skip + i)))
    in_specs = [
        FIRST,
        pl.BlockSpec(block, lambda i, at: spot(axis, skip + i)),
        pl.BlockSpec((1, *block), lambda i, at: (l, 3 * at[0] + skip + i, 0) if axis == 0 else (l, at[0], skip + i)),
        moment,
        moment,
    ]
    args = [factor, g, w, m, v]
    aliases = {}
    if so_far is not None:
        in_specs += [ANY, ANY]
        args += so_far
        aliases = {6: 1, 7: 2}
    new = tuple(n * count if k == axis else n for k, n in enumerate(block))
    return pl.pallas_call(
        adamw_kernel,
        grid_spec=pltpu.PrefetchScalarGridSpec(
            num_scalar_prefetch=1,
            grid=(count,),
            in_specs=in_specs,
            out_specs=[pl.BlockSpec(block, lambda i, at: spot(axis, i)), moment, moment],
        ),
        out_shape=[jax.ShapeDtypeStruct(new, BF)] + [jax.ShapeDtypeStruct(m.shape, F32)] * 2,
        input_output_aliases=aliases,
        compiler_params=pltpu.CompilerParams(vmem_limit_bytes=SMALL_LIMIT),
        cost_estimate=cost(0.1, m.size),
    )(at, *args)


def adamw_ahead_kernel(owners_ref, f_ref, g_ref, w_ref, m_ref, v_ref, nw_ref):
    factor = f_ref[:1, :1]

    @pl.loop(0, PART // 32)
    def _(i):
        r = pl.ds(pl.multiple_of(i * 32, 32), 32)
        nw_ref[0, r, :], _, _ = stepped(factor, g_ref[r, :], w_ref[0, r, :], m_ref[r, :], v_ref[r, :])


def adamw_ahead(owners, factor, g, w, mv):
    block = (PART, BLOCK)
    return pl.pallas_call(
        adamw_ahead_kernel,
        grid_spec=pltpu.PrefetchScalarGridSpec(
            num_scalar_prefetch=1,
            grid=(3, TILES),
            in_specs=[
                FIRST,
                pl.BlockSpec((SQUEEZED, SQUEEZED, *block), lambda s, t, own: (s, t, 0, 0)),
                pl.BlockSpec((1, *block), lambda s, t, own: (1, own[s], t)),
                *[pl.BlockSpec((SQUEEZED, SQUEEZED, *block), lambda s, t, own, k=k: (k, s, 0, t)) for k in range(2)],
            ],
            out_specs=pl.BlockSpec((1, *block), lambda s, t, own: (s, 0, t)),
        ),
        out_shape=jax.ShapeDtypeStruct((3, PART, AHEAD), BF),
        compiler_params=pltpu.CompilerParams(vmem_limit_bytes=SMALL_LIMIT),
        cost_estimate=cost(0.1, 14 * 3 * PART * AHEAD),
        name="adamw_ahead",
    )(owners, factor, g, w, mv, mv)


def place_kernel(n, owners_ref, *refs):
    out_ref = refs[-1]
    s = pl.program_id(0)
    for k in range(n):

        @pl.when(s == k)
        def _():
            out_ref[0] = refs[k][...]


def place(piece, owners, pieces, so_far, whole):
    _, l, axis, skip, count = piece
    n = len(pieces)
    block = tuple(m // count if k == axis else m for k, m in enumerate(pieces[0].shape))

    def of(k):
        return lambda s, i, own: spot(axis, jnp.where(s == k, i, jnp.where(s < k, 0, count - 1)))

    in_specs = [pl.BlockSpec(block, of(k)) for k in range(n)]
    args = list(pieces)
    aliases = {}
    if so_far is not None:
        in_specs.append(ANY)
        args.append(so_far)
        aliases = {n + 1: 0}
    return pl.pallas_call(
        functools.partial(place_kernel, n),
        grid_spec=pltpu.PrefetchScalarGridSpec(
            num_scalar_prefetch=1,
            grid=(n, count),
            in_specs=in_specs,
            out_specs=pl.BlockSpec(
                (1, *block), lambda s, i, own: (l, 3 * own[s] + skip + i, 0) if axis == 0 else (l, own[s], skip + i)
            ),
        ),
        out_shape=jax.ShapeDtypeStruct(whole.shape, BF),
        input_output_aliases=aliases,
        compiler_params=pltpu.CompilerParams(vmem_limit_bytes=SMALL_LIMIT),
        cost_estimate=cost(0.1, whole.size),
    )(owners, *args)


def place_ahead_kernel(owners_ref, new_ref, so_far, out_ref):
    out_ref[...] = new_ref[...]


def place_ahead(owners, new, so_far):
    block = (1, PART, THIRD)
    return pl.pallas_call(
        place_ahead_kernel,
        grid_spec=pltpu.PrefetchScalarGridSpec(
            num_scalar_prefetch=1,
            grid=(3, 2),
            in_specs=[pl.BlockSpec(block, lambda s, i, own: (s, 0, i)), ANY],
            out_specs=pl.BlockSpec(block, lambda s, i, own: (1, own[s], i)),
        ),
        out_shape=jax.ShapeDtypeStruct(so_far.shape, BF),
        input_output_aliases={2: 0},
        compiler_params=pltpu.CompilerParams(vmem_limit_bytes=SMALL_LIMIT),
        cost_estimate=cost(0.1, 4 * 3 * PART * AHEAD),
        name="place_ahead",
    )(owners, new, so_far)


PIECES = [(GATE, 1, 1, 2, 1)] + [(GATE, 0, 1, n, 1) for n in range(3)]
PIECES += [(n, l, 0, *part) for n, part in ((UP, (0, 3)), (DOWN, (0, 2)), (DOWN, (2, 1))) for l in range(LAYERS)]
KNOWN = (0, 1, 1, 0, 2)


def solution(mesh):
    def swap(t, mask):
        return lax.ppermute(t, "dp", [(i, i ^ mask) for i in range(8)])

    def step(x, dy, wg, wu, wd, mg, mu, md, vg, vu, vd):
        x, dy = x[0], dy[0]
        me = lax.axis_index("dp")
        a, ht, sl, q, h1, mv = forward(x, wg, wu, wd, mg, vg)
        *g1, squares, dh1, g_ahead = backward(1, Lags(1, 2, 2, 2), a, dy, wd, sl, q, ht, wg, wu, h1)
        *g0, factor = backward(0, Lags(2, 4, 3, 3), a, dh1, wd, sl, q, ht, squares)
        at = me[None].astype(jnp.int32)
        groups = {name: jnp.stack([me ^ k for k in group]).astype(jnp.int32) for name, group in GROUPS.items()}
        mats = ((wg, mg, vg), (wu, mu, vu), (wd, md, vd))
        moments, whole = [None] * 3, [None] * 3

        def put(kind, piece, have):
            n = piece[0]
            whole[n] = place(piece, groups[kind], [have[k] for k in GROUPS[kind]], whole[n], mats[n][0])

        def new_rows(piece):
            n, l = piece[:2]
            new, *moments[n] = adamw(piece, at, factor, (g0, g1)[l][n], *mats[n], moments[n])
            return new

        everything = []
        for number, piece in enumerate(PIECES):
            have = {}
            everything.append(have)
            have[0] = new_rows(piece)
            have[4] = swap(have[0], 4)
            have[2] = swap(have[0], 2)
            have[6] = swap(have[4], 2) if number % 2 else swap(have[2], 4)
            for k in (0, 4, 2, 6):
                have[k + 1] = swap(have[k], 1)
            put("own", piece, have)
            put("near", piece, have)
        have = {0: new_rows(KNOWN)}
        have[1] = swap(have[0], 1)
        put("own", KNOWN, have)
        ahead = adamw_ahead(groups["ahead_own"], factor, g_ahead, wg, mv)
        for kind, new in (("ahead_own", ahead), ("ahead_partner", swap(ahead, 1))):
            whole[0] = place_ahead(groups[kind], new, whole[0])
        for piece, have in zip(PIECES, everything):
            put("across", piece, have)
            put("last", piece, have)
        return tuple(whole + [m[0] for m in moments] + [m[1] for m in moments])

    whole, rows = P(), P(None, "dp")
    return jax.shard_map(
        step,
        mesh=mesh,
        in_specs=(P(("rep", "dp")),) * 2 + (whole,) * 3 + (rows,) * 6,
        out_specs=(P("rep"),) * 3 + (P("rep", "dp"),) * 6,
        check_vma=False,
    )
```

```python
import functools

import jax
import jax.numpy as jnp
from jax import lax
from jax.experimental import pallas as pl
from jax.experimental.pallas import tpu as pltpu
from jax.sharding import PartitionSpec as P


BF = jnp.bfloat16
F32 = jnp.float32
MESH = pl.DeviceIdType.MESH
TOKENS, D, FF, LAYERS = 2048, 1536, 4224, 2
BLOCK = 256
STEPS = -(-FF // BLOCK)
LAST = FF - (STEPS - 1) * BLOCK
ALL = LAYERS * STEPS
PART = D // 8
SUB = BLOCK // 8
OWN_DOWN = FF // 8
LAST_SUB = OWN_DOWN - (STEPS - 1) * SUB
HALF = PART // 2
CHUNK = PART + HALF
COUNT = 3 * LAYERS * D * FF
THIRD = FF // 3
GATE, UP, DOWN = range(3)
AHEAD = 2 * THIRD
TILES = AHEAD // BLOCK
SPREAD = 13
VMEM_LIMIT = 67043328
SMALL_LIMIT = 48 << 20


ANY = pl.BlockSpec(memory_space=pl.ANY)
SQUEEZED = pl.Squeezed()
FACTOR = (8, 128)
FIRST = pl.BlockSpec(FACTOR, lambda *_: (0, 0))
GROUPS = {"own": (0, 1), "near": (4, 2, 5, 3), "across": (6,), "last": (7,), "ahead_own": (4, 2, 6), "ahead_partner": (5, 3, 7)}


def dot(a, b, dims="nn"):
    ca, cb = ("tn".index(dims[0]), "nt".index(dims[1]))
    return lax.dot_general(a, b, (((ca,), (cb,)), ((), ())), preferred_element_type=F32)


def resident(shape):
    return pl.BlockSpec(shape, lambda *_: (0,) * len(shape), pipeline_mode=pl.Buffered(1))


def cost(units, bytes_accessed):
    return pl.CostEstimate(flops=int(units * 2 * TOKENS * D * FF), bytes_accessed=int(bytes_accessed), transcendentals=0)


def normed(h):
    wide = h.astype(F32)
    scale = lax.rsqrt(jnp.mean(wide * wide, -1, keepdims=True) + 1e-6)
    return (wide * scale).astype(BF)


def neighbours():
    me = lax.axis_index("dp")
    x, y, c = lax.div(me, 4), lax.rem(lax.div(me, 2), 2), lax.rem(me, 2)
    return (me, x, y, c), [{"dp": me + k * (1 - 2 * t)} for k, t in ((1, c), (4, x), (2, y))]


def remote(src, dst, send, recv, to):
    return pltpu.make_async_remote_copy(src_ref=src, dst_ref=dst, send_sem=send, recv_sem=recv, device_id=to, device_id_type=MESH)


class Weights:
    def __init__(self, l, wg, wu, wd, gu_ref, down_ref, sems):
        self.l, self.wg, self.wu, self.wd, self.gu_ref, self.down_ref, self.sems = l, wg, wu, wd, gu_ref, down_ref, sems

    def copies(self, j, last):
        slot, block, l = lax.rem(j, 2), lax.rem(j, STEPS), self.l
        if l is None:
            l = lax.div(j, STEPS)
        width = LAST if last else BLOCK
        start = (STEPS - 1) * BLOCK if last else pl.multiple_of(block * BLOCK, BLOCK)
        columns = pl.ds(start, width)
        pairs = [
            (self.wg.at[l, :, columns], self.gu_ref.at[slot, :, pl.ds(0, width)]),
            (self.wu.at[l, :, columns], self.gu_ref.at[slot, :, pl.ds(BLOCK, width)]),
        ]
        if self.wd is not None:
            pairs.append((self.wd.at[l, columns], self.down_ref.at[slot, pl.ds(0, width)]))
        return [pltpu.make_async_copy(src, dst, self.sems.at[slot, n]) for n, (src, dst) in enumerate(pairs)]

    def each(self, j, act):
        block = lax.rem(j, STEPS)

        @pl.when(block < STEPS - 1)
        def _():
            for copy in self.copies(j, False):
                act(copy)

        @pl.when(block == STEPS - 1)
        def _():
            for copy in self.copies(j, True):
                act(copy)

    def start(self, j):
        self.each(j, lambda copy: copy.start())

    def wait(self, j):
        self.each(j, lambda copy: copy.wait())


def forward_kernel(x_ref, wg, wu, wd, m_in, v_in, *refs):
    a_out, ht_ref, sl_ref, q_ref, h_out, mv_out, *refs = refs
    a_ref, h_ref, gu_ref, down_ref, hid_ref, acc_ref, w_sems, sems, near_send, near_recv, far_send, far_recv = refs
    j = pl.program_id(0)
    block = lax.rem(j, STEPS)
    weights = Weights(None, wg, wu, wd, gu_ref, down_ref, w_sems)
    _, (_, to_x, to_y) = neighbours()
    barrier = pltpu.get_barrier_semaphore()
    keep = [pltpu.make_async_copy(a_ref, a_out.at[l], sems.at[l]) for l in range(LAYERS)]
    keep_h = pltpu.make_async_copy(h_ref, h_out, sems.at[2])

    def near(k):
        src = (m_in, v_in)[k].at[1, :, pl.ds(0, AHEAD)]
        return [remote(src, mv_out.at[k, n], near_send.at[k, n], near_recv.at[k, n], to) for n, to in enumerate((to_x, to_y))]

    def far(k):
        return [
            remote(mv_out.at[k, n, rows], mv_out.at[k, 2, rows], far_send.at[k, n], far_recv.at[k, n], to)
            for n, (rows, to) in enumerate(((pl.ds(0, HALF), to_y), (pl.ds(HALF, HALF), to_x)))
        ]

    @pl.when(j == 0)
    def _():
        for to in (to_x, to_y):
            pl.semaphore_signal(barrier, inc=1, device_id=to, device_id_type=MESH)
        weights.start(j)

        @pl.loop(0, TOKENS // 256)
        def _(i):
            r = pl.ds(pl.multiple_of(i * 256, 256), 256)
            a_ref[r, :] = normed(x_ref[r, :])
            acc_ref[r, :] = jnp.zeros((256, D), F32)

        keep[0].start()

    @pl.when(j == 2)
    def _():
        pl.semaphore_wait(barrier, 2)
        for k in range(2):
            for copy in near(k):
                copy.start()

    @pl.when(j == STEPS)
    def _():
        keep[0].wait()

        @pl.loop(0, TOKENS // 256)
        def _(i):
            r = pl.ds(pl.multiple_of(i * 256, 256), 256)
            h = x_ref[r, :] + acc_ref[r, :].astype(BF)
            h_ref[r, :] = h
            a_ref[r, :] = normed(h)

        keep[1].start()
        keep_h.start()

    @pl.when(j == STEPS + 4)
    def _():
        for k in range(2):
            for copy in near(k):
                copy.wait()
            for copy in far(k):
                copy.start()

    pl.when(j + 1 < ALL)(lambda: weights.start(j + 1))
    weights.wait(j)
    slot = lax.rem(j, 2)
    for i in range(8):
        r = slice(256 * i, 256 * i + 256)
        gu = dot(a_ref[r, :], gu_ref[slot])
        g, u = gu[:, :BLOCK], gu[:, BLOCK:]
        s = jax.nn.sigmoid(g)
        sl = g * s
        sl_ref[0, r, :] = sl
        q_ref[0, r, :] = u * (s * (1.0 + g * (1.0 - s)))
        hid = (sl * u).astype(BF)
        hid_ref[r, :] = hid
        ht_ref[0, :, r] = hid.T

    @pl.when(j < STEPS)
    def _():
        @pl.when(block == STEPS - 1)
        def _():
            hid_ref[:, LAST:] = jnp.zeros((TOKENS, BLOCK - LAST), BF)

        acc_ref[...] += dot(hid_ref[...], down_ref[slot])

    @pl.when(j == ALL - 1)
    def _():
        keep[1].wait()
        keep_h.wait()
        for k in range(2):
            for copy in far(k):
                copy.wait()


def forward(x, wg, wu, wd, m, v):
    layer = lambda j: lax.div(j, STEPS)
    block = lambda j: lax.rem(j, STEPS)
    wide = pl.BlockSpec((1, TOKENS, BLOCK), lambda j: (layer(j), 0, block(j)))
    shape = jax.ShapeDtypeStruct
    return pl.pallas_call(
        forward_kernel,
        grid=(ALL,),
        in_specs=[resident((TOKENS, D))] + [ANY] * 5,
        out_specs=[ANY, pl.BlockSpec((1, BLOCK, TOKENS), lambda j: (layer(j), block(j), 0)), wide, wide, ANY, ANY],
        out_shape=[
            shape((LAYERS, TOKENS, D), BF),
            shape((LAYERS, FF, TOKENS), BF),
            *[shape((LAYERS, TOKENS, FF), F32)] * 2,
            shape((TOKENS, D), BF),
            shape((2, 3, PART, AHEAD), F32),
        ],
        scratch_shapes=[
            pltpu.VMEM((TOKENS, D), BF),
            pltpu.VMEM((TOKENS, D), BF),
            pltpu.VMEM((2, D, 2 * BLOCK), BF),
            pltpu.VMEM((2, BLOCK, D), BF),
            pltpu.VMEM((TOKENS, BLOCK), BF),
            pltpu.VMEM((TOKENS, D), F32),
            pltpu.SemaphoreType.DMA((2, 3)),
            pltpu.SemaphoreType.DMA((3,)),
            *[pltpu.SemaphoreType.DMA((2, 2))] * 4,
        ],
        compiler_params=pltpu.CompilerParams(vmem_limit_bytes=VMEM_LIMIT, collective_id=1, has_side_effects=True),
        cost_estimate=cost(5, 260e6),
        name="forward",
    )(x, wg, wu, wd, m, v)


def bits(o):
    return o // 4, o // 2 % 2, o % 2


class Lags:
    def __init__(self, second, third, b, e):
        self.second, self.third, self.b, self.e = second, third, b, e
        self.s = third + 1
        self.a = third + 2
        self.c = second + third
        self.d = 2 * (third - second)


def backward_kernel(lags, a_in, dy_in, wd_ref, sl_ref, q_ref, ht_ref, wg, wu, h_in, *refs):
    g_gate, g_up, g_down, f_ref, far_out, acc_ref, gu_ref, w_sems, sq_ref, every_ref, f_send, f_recv, *refs = refs
    near_send, near_recv, far_send, far_recv, a_ref, dy_ref, dgu_ref, s_ref, a2_ref, bx, by, cx, cy, ex, ey, dx, dy2, *refs = refs
    og, ou, od, s_send, a_recv, bx_send, by_send, cx_recv, cy_recv, ex_send, ey_send, dx_recv, dy_recv, out_sem, a_sem = refs
    weights = Weights(1, wg, wu, None, gu_ref, None, w_sems)
    j = pl.program_id(0)
    block = lax.rem(j, STEPS)
    (me, x, y, c), (to_core, to_x, to_y) = neighbours()
    xn, yn, cn = (1 - k for k in (x, y, c))
    others = [{"dp": lax.rem(me + k, 8)} for k in range(1, 8)]

    def columns(last):
        return pl.ds(0, LAST if last else BLOCK)

    def pair(i, last, which=(0, 1)):
        s, a, w = lax.rem(i, lags.s), lax.rem(i, lags.a), columns(last)
        return [
            remote(s_ref.at[s, n, :, :, cn, :, w], a2_ref.at[a, n, :, :, :, w], s_send.at[s, k], a_recv.at[a, k], to_core)
            for k, n in ((k, (pl.ds(0, 2), pl.ds(2, 1))[k]) for k in which)
        ]

    def first(i, last):
        b, k, w = lax.rem(i, lags.b), lax.rem(i, lags.c), columns(last)
        return [
            remote(bx.at[b, :, :, w], cx.at[k, :, :, w], bx_send.at[b], cx_recv.at[k], to_x),
            remote(by.at[b, :, :, w], cy.at[k, :, :, w], by_send.at[b], cy_recv.at[k], to_y),
        ]

    def second(i, last):
        e, k, w = lax.rem(i, lags.e), lax.rem(i, lags.d), columns(last)
        return [
            remote(ex.at[e, :, w], dx.at[k, :, w], ex_send.at[e], dx_recv.at[k], to_x),
            remote(ey.at[e, :, w], dy2.at[k, :, w], ey_send.at[e], dy_recv.at[k], to_y),
        ]

    def outs(i, last):
        o, p, l, n = lax.rem(i, 2), lax.rem(i, og.shape[0]), 1 - lax.div(i, STEPS), lax.rem(i, STEPS)
        w = columns(last)
        wide = pl.ds(pl.multiple_of(n * BLOCK, BLOCK), w.size)
        deep = pl.ds(pl.multiple_of(n * SUB, SUB), LAST_SUB if last else SUB)
        srcs = og.at[p, :, w], ou.at[o, :, w], od.at[o, pl.ds(0, deep.size)]
        dsts = g_gate.at[l, :, wide], g_up.at[l, :, wide], g_down.at[l, deep]
        return [pltpu.make_async_copy(s, d, out_sem.at[o, n]) for n, (s, d) in enumerate(zip(srcs, dsts))]

    def each(i, copies, act):
        last = lax.rem(i, STEPS) == STEPS - 1

        @pl.when(jnp.logical_not(last))
        def _():
            for copy in copies(i, False):
                act(copy)

        @pl.when(last)
        def _():
            for copy in copies(i, True):
                act(copy)

    def start(copy):
        copy.start()

    def total(*terms):
        return functools.reduce(lambda p, q: p + q, [t.astype(F32) for t in terms])

    def take_first(i):
        each(i, pair, lambda copy: copy.wait())
        s, a, b = lax.rem(i, lags.s), lax.rem(i, lags.a), lax.rem(i, lags.b)

        pl.when(i >= lags.b)(lambda: each(i - lags.b, first, lambda copy: copy.wait_send()))

        for t in range(2):
            bx[b, t, :PART] = total(s_ref[s, GATE, xn, t, c], a2_ref[a, GATE, xn, t]).astype(BF)
            bx[b, t, PART:] = total(s_ref[s, DOWN, xn, t, c, :HALF], a2_ref[a, DOWN, xn, t, :HALF]).astype(BF)
            by[b, t, :PART] = total(s_ref[s, UP, t, yn, c], a2_ref[a, UP, t, yn]).astype(BF)
            by[b, t, PART:] = total(s_ref[s, DOWN, t, yn, c, HALF:], a2_ref[a, DOWN, t, yn, HALF:]).astype(BF)
        each(i, first, start)

    def take_second(i):
        each(i, first, lambda copy: copy.wait_recv())
        s, a, k, e = lax.rem(i, lags.s), lax.rem(i, lags.a), lax.rem(i, lags.c), lax.rem(i, lags.e)

        pl.when(i >= lags.e)(lambda: each(i - lags.e, second, lambda copy: copy.wait_send()))

        ey[e, :PART] = total(s_ref[s, GATE, x, yn, c], a2_ref[a, GATE, x, yn], cx[k, yn, :PART]).astype(BF)
        ey[e, PART:] = total(s_ref[s, DOWN, x, yn, c, :HALF], a2_ref[a, DOWN, x, yn, :HALF], cx[k, yn, PART:]).astype(BF)
        ex[e, :PART] = total(s_ref[s, UP, xn, y, c], a2_ref[a, UP, xn, y], cy[k, xn, :PART]).astype(BF)
        ex[e, PART:] = total(s_ref[s, DOWN, xn, y, c, HALF:], a2_ref[a, DOWN, xn, y, HALF:], cy[k, xn, PART:]).astype(BF)
        each(i, second, start)

    def take_third(i):
        each(i, second, lambda copy: copy.wait_recv())
        s, a, k, d, o = (lax.rem(i, n) for n in (lags.s, lags.a, lags.c, lags.d, 2))

        pl.when(i >= 1)(lambda: each(i - 1, outs, lambda copy: copy.wait()))

        gate = total(s_ref[s, GATE, x, y, c], a2_ref[a, GATE, x, y], cx[k, y, :PART], dy2[d, :PART]).astype(BF)
        up = total(s_ref[s, UP, x, y, c], a2_ref[a, UP, x, y], cy[k, x, :PART], dx[d, :PART]).astype(BF)
        og[lax.rem(i, og.shape[0])] = gate
        ou[o] = up
        low = total(s_ref[s, DOWN, x, y, c, :HALF], a2_ref[a, DOWN, x, y, :HALF], cx[k, y, PART:], dy2[d, PART:]).astype(BF)
        high = total(s_ref[s, DOWN, x, y, c, HALF:], a2_ref[a, DOWN, x, y, HALF:], cy[k, x, PART:], dx[d, PART:]).astype(BF)
        downs = [half[SUB * n : SUB * n + SUB] for half in (low, high) for n in range(HALF // SUB)]

        def squares(t):
            wide = t.astype(F32)
            return jnp.sum((wide * wide).reshape(-1, 8, t.shape[-1]), 0)

        last = lax.rem(i, STEPS) == STEPS - 1

        @pl.when(jnp.logical_not(last))
        def _():
            for n, one in enumerate(downs):
                od[o, :, BLOCK * n : BLOCK * n + BLOCK] = one
            sq_ref[...] += squares(gate) + squares(up) + squares(low) + squares(high)

        @pl.when(last)
        def _():
            for n, one in enumerate(downs):
                od[o, :LAST_SUB, BLOCK * n : BLOCK * n + LAST] = one[:LAST_SUB, :LAST]
                od[o, :LAST_SUB, BLOCK * n + LAST : BLOCK * n + BLOCK] = one[LAST_SUB:, :LAST]
            sq_ref[:, :LAST] += sum(squares(t[:, :LAST]) for t in (gate, up, low, high))

        each(i, outs, start)

    def near(t):
        k = lax.rem(t, 4)
        src = og.at[lax.rem(t, og.shape[0])]
        return [remote(src, far_out.at[n, t], near_send.at[k, n], near_recv.at[k, n], to) for n, to in enumerate((to_x, to_y))]

    def far(t):
        k = lax.rem(t, 4)
        return [
            remote(far_out.at[n, t, rows], far_out.at[2, t, rows], far_send.at[k, n], far_recv.at[k, n], to)
            for n, (rows, to) in enumerate(((pl.ds(0, HALF), to_y), (pl.ds(HALF, HALF), to_x)))
        ]

    def at_step(n, act):
        t = lax.div(n * TILES, SPREAD)

        @pl.when((n >= 0) & (n < SPREAD) & ((n == 0) | (t > lax.div((n - 1) * TILES, SPREAD))))
        def _():
            act(t)

    def pass_on(t):
        for copy in near(t):
            copy.wait()
        for copy in far(t):
            copy.start()

    take_a1, take_a0 = (pltpu.make_async_copy(a_in.at[l], a_ref, a_sem.at[l]) for l in (1, 0))
    take_h = pltpu.make_async_copy(h_in, a_ref, a_sem.at[2])
    take_dy = pltpu.make_async_copy(dy_in, dy_ref, a_sem.at[3])
    barrier = pltpu.get_barrier_semaphore()

    @pl.when(j == 0)
    def _():
        take_dy.start()
        take_a1.start()
        weights.start(j)
        for to in others:
            pl.semaphore_signal(barrier, inc=1, device_id=to, device_id_type=MESH)
        sq_ref[...] = jnp.zeros_like(sq_ref)

        @pl.loop(0, TOKENS // 256)
        def _(i):
            acc_ref[pl.ds(pl.multiple_of(i * 256, 256), 256), :] = jnp.zeros((256, D), F32)

        take_dy.wait()

    @pl.when(j == STEPS)
    def _():
        take_h.wait()

        @pl.loop(0, TOKENS // 128)
        def _(i):
            r = pl.ds(pl.multiple_of(i * 128, 128), 128)
            h = a_ref[r, :].astype(F32)
            da = acc_ref[r, :].astype(BF).astype(F32)
            scale = lax.rsqrt(jnp.mean(h * h, -1, keepdims=True) + 1e-6)
            along = jnp.sum(da * h, -1, keepdims=True) * (scale * scale * scale) * (1.0 / D)
            dy_ref[r, :] = dy_ref[r, :] + (da * scale - h * along).astype(BF)

        take_a0.start()

    @pl.when(j < ALL)
    def _():
        pl.when(j + 1 < STEPS)(lambda: weights.start(j + 1))
        s = lax.rem(j, lags.s)
        for i in range(4):
            r = slice(512 * i, 512 * i + 512)
            dh = dot(dy_ref[r, :], wd_ref[0], "nt").astype(BF).astype(F32)
            dgu_ref[r, :BLOCK] = (dh * q_ref[0, r, :]).astype(BF)
            dgu_ref[r, BLOCK:] = (dh * sl_ref[0, r, :]).astype(BF)

        pl.when(j == 0)(lambda: take_a1.wait())
        pl.when(j == STEPS)(lambda: take_a0.wait())

        @pl.when(block == STEPS - 1)
        def _():
            dgu_ref[:, LAST:BLOCK] = jnp.zeros((TOKENS, BLOCK - LAST), BF)
            dgu_ref[:, BLOCK + LAST :] = jnp.zeros((TOKENS, BLOCK - LAST), BF)

        for h in range(2):
            gu = dot(a_ref[:, D // 2 * h : D // 2 * (h + 1)], dgu_ref[...], "tn")
            for o in range(4):
                for t in range(2):
                    s_ref[s, t, h, o // 2, o % 2] = gu[PART * o : PART * o + PART, BLOCK * t : BLOCK * t + BLOCK].astype(BF)
        pl.when(j == STEPS - 1)(lambda: take_h.start())
        pl.when(j == 0)(lambda: pl.semaphore_wait(barrier, len(others)))
        each(j, functools.partial(pair, which=(0,)), start)
        for h in range(2):
            down = dot(ht_ref[...].reshape(BLOCK, TOKENS), dy_ref[:, D // 2 * h : D // 2 * (h + 1)])
            for o in range(8):
                for n in range(3):
                    s_ref[(s, DOWN, *bits(o), slice(SUB * (3 * h + n), SUB * (3 * h + n + 1)))] = down[
                        SUB * o : SUB * o + SUB, BLOCK * n : BLOCK * n + BLOCK
                    ].astype(BF)

        @pl.when(block == STEPS - 1)
        def _():
            for o in range(8):
                for n in range(6):
                    half = SUB * n + LAST_SUB
                    s_ref[(s, DOWN, *bits(o), slice(half, SUB * n + SUB), slice(LAST))] = s_ref[
                        (s, DOWN, *bits(o), slice(SUB * n, half), slice(LAST, BLOCK))
                    ]

        each(j, functools.partial(pair, which=(1,)), start)

        @pl.when(j < STEPS)
        def _():
            weights.wait(j)
            for i in range(8):
                r = slice(256 * i, 256 * i + 256)
                acc_ref[r, :] += dot(dgu_ref[r, :], gu_ref[lax.rem(j, 2)], "nt")

    pl.when((j >= lags.third) & (j < ALL + lags.third))(lambda: take_third(j - lags.third))
    pl.when((j >= lags.second) & (j < ALL + lags.second))(lambda: take_second(j - lags.second))
    pl.when(j < ALL)(lambda: take_first(j))
    at_step(j - lags.third - 4, lambda t: [copy.wait() for copy in far(t)])
    at_step(j - lags.third - 2, pass_on)
    at_step(j - lags.third, lambda t: [copy.start() for copy in near(t)])

    @pl.when(j == ALL + lags.third - 1)
    def _():
        both = sq_ref[...]
        every_ref[me] = both[:, :128] + both[:, 128:]

        def exchange():
            return [remote(every_ref.at[me], every_ref.at[me], f_send.at[n], f_recv.at[n], to) for n, to in enumerate(others)]

        for copy in exchange():
            copy.start()
        for i in range(ALL - lags.b, ALL):
            for copy in first(jnp.int32(i), i == ALL - 1):
                copy.wait_send()
        for i in range(ALL - lags.e, ALL):
            for copy in second(jnp.int32(i), i == ALL - 1):
                copy.wait_send()
        for copy in outs(jnp.int32(ALL - 1), True):
            copy.wait()
        for copy in exchange():
            copy.wait()
        squares = functools.reduce(lambda p, q: p + q, [every_ref[n] for n in range(8)])
        squares = jnp.sum(jnp.sum(squares, axis=1, keepdims=True), axis=0, keepdims=True)
        f_ref[...] = jnp.broadcast_to(jnp.minimum(1.0, 0.5 * lax.rsqrt(squares / COUNT + 1e-30)), FACTOR)


def backward(lags, a, dy, wd, sl, q, ht, wg, wu, h):
    layer = lambda j: 1 - lax.div(jnp.minimum(j, ALL - 1), STEPS)
    block = lambda j: lax.rem(jnp.minimum(j, ALL - 1), STEPS)
    wide = pl.BlockSpec((1, TOKENS, BLOCK), lambda j: (layer(j), 0, block(j)))
    shape = jax.ShapeDtypeStruct
    piece = (PART, BLOCK)
    dma = pltpu.SemaphoreType.DMA
    return pl.pallas_call(
        functools.partial(backward_kernel, lags),
        grid=(ALL + lags.third,),
        in_specs=[
            ANY,
            ANY,
            pl.BlockSpec((1, BLOCK, D), lambda j: (layer(j), block(j), 0)),
            wide,
            wide,
            pl.BlockSpec((8, SUB, TOKENS), lambda j: (layer(j), block(j), 0)),
            ANY,
            ANY,
            ANY,
        ],
        out_specs=[ANY, ANY, ANY, FIRST, ANY],
        out_shape=[
            *[shape((LAYERS, PART, FF), BF)] * 2,
            shape((LAYERS, OWN_DOWN, D), BF),
            shape(FACTOR, F32),
            shape((3, TILES, *piece), BF),
        ],
        scratch_shapes=[
            pltpu.VMEM((TOKENS, D), F32),
            pltpu.VMEM((2, D, 2 * BLOCK), BF),
            dma((2, 3)),
            pltpu.VMEM((8, BLOCK), F32),
            pltpu.VMEM((8, *FACTOR), F32),
            *[dma((7,))] * 2,
            *[dma((4, 2))] * 4,
            *[pltpu.VMEM((TOKENS, D), BF)] * 2,
            pltpu.VMEM((TOKENS, 2 * BLOCK), BF),
            pltpu.VMEM((lags.s, 3, 2, 2, 2, *piece), BF),
            pltpu.VMEM((lags.a, 3, 2, 2, *piece), BF),
            *[pltpu.VMEM((n, 2, CHUNK, BLOCK), BF) for n in (lags.b, lags.b, lags.c, lags.c)],
            *[pltpu.VMEM((n, CHUNK, BLOCK), BF) for n in (lags.e, lags.e, lags.d, lags.d)],
            *[pltpu.VMEM((n, *piece), BF) for n in (5, 2)],
            pltpu.VMEM((2, SUB, D), BF),
            *[dma((n, 2)) for n in (lags.s, lags.a)],
            *[dma((n,)) for n in (lags.b, lags.b, lags.c, lags.c, lags.e, lags.e, lags.d, lags.d)],
            dma((2, 3)),
            dma((4,)),
        ],
        compiler_params=pltpu.CompilerParams(vmem_limit_bytes=VMEM_LIMIT, collective_id=0, has_side_effects=True),
        cost_estimate=cost(10, 300e6),
        name="backward",
    )(a, dy, wd, sl, q, ht.reshape(LAYERS * 8, OWN_DOWN, TOKENS), wg, wu, h)


def stepped(factor, g, w, m, v):
    g, w = g.astype(F32) * factor, w.astype(F32)
    m = 0.9 * m + 0.1 * g
    v = 0.95 * v + 0.05 * g * g
    return (w - 0.02 * (m * lax.rsqrt(v + 1e-8) + 0.1 * w)).astype(BF), m, v


def adamw_kernel(at_ref, f_ref, g_ref, w_ref, m_ref, v_ref, *refs):
    nw_ref, nm_ref, nv_ref = refs[-3:]
    factor = f_ref[:1, :1]

    @pl.loop(0, g_ref.shape[0] // 16)
    def _(i):
        r = pl.ds(pl.multiple_of(i * 16, 16), 16)
        nw_ref[r, :], nm_ref[0, r, :], nv_ref[0, r, :] = stepped(factor, g_ref[r, :], w_ref[0, r, :], m_ref[0, r, :], v_ref[0, r, :])


def thirds(shape, axis):
    return tuple(n // 3 if k == axis else n for k, n in enumerate(shape))


def spot(axis, i, other=0):
    return (i, other) if axis == 0 else (other, i)


def adamw(piece, at, factor, g, w, m, v, so_far=None):
    _, l, axis, skip, count = piece
    block = thirds(g.shape[1:], axis)
    moment = pl.BlockSpec((1, *block), lambda i, at: (l, *spot(axis, skip + i)))
    in_specs = [
        FIRST,
        pl.BlockSpec((SQUEEZED, *block), lambda i, at: (l, *spot(axis, skip + i))),
        pl.BlockSpec((1, *block), lambda i, at: (l, 3 * at[0] + skip + i, 0) if axis == 0 else (l, at[0], skip + i)),
        moment,
        moment,
    ]
    args = [factor, g, w, m, v]
    aliases = {}
    if so_far is not None:
        in_specs += [ANY, ANY]
        args += so_far
        aliases = {6: 1, 7: 2}
    new = tuple(n * count if k == axis else n for k, n in enumerate(block))
    return pl.pallas_call(
        adamw_kernel,
        grid_spec=pltpu.PrefetchScalarGridSpec(
            num_scalar_prefetch=1,
            grid=(count,),
            in_specs=in_specs,
            out_specs=[pl.BlockSpec(block, lambda i, at: spot(axis, i)), moment, moment],
        ),
        out_shape=[jax.ShapeDtypeStruct(new, BF)] + [jax.ShapeDtypeStruct(m.shape, F32)] * 2,
        input_output_aliases=aliases,
        compiler_params=pltpu.CompilerParams(vmem_limit_bytes=SMALL_LIMIT),
        cost_estimate=cost(0.1, m.size),
    )(at, *args)


def adamw_ahead_kernel(owners_ref, f_ref, g_ref, w_ref, m_ref, v_ref, nw_ref):
    factor = f_ref[:1, :1]

    @pl.loop(0, PART // 32)
    def _(i):
        r = pl.ds(pl.multiple_of(i * 32, 32), 32)
        nw_ref[0, r, :], _, _ = stepped(factor, g_ref[r, :], w_ref[0, r, :], m_ref[r, :], v_ref[r, :])


def adamw_ahead(owners, factor, g, w, mv):
    block = (PART, BLOCK)
    return pl.pallas_call(
        adamw_ahead_kernel,
        grid_spec=pltpu.PrefetchScalarGridSpec(
            num_scalar_prefetch=1,
            grid=(3, TILES),
            in_specs=[
                FIRST,
                pl.BlockSpec((SQUEEZED, SQUEEZED, *block), lambda s, t, own: (s, t, 0, 0)),
                pl.BlockSpec((1, *block), lambda s, t, own: (1, own[s], t)),
                *[pl.BlockSpec((SQUEEZED, SQUEEZED, *block), lambda s, t, own, k=k: (k, s, 0, t)) for k in range(2)],
            ],
            out_specs=pl.BlockSpec((1, *block), lambda s, t, own: (s, 0, t)),
        ),
        out_shape=jax.ShapeDtypeStruct((3, PART, AHEAD), BF),
        compiler_params=pltpu.CompilerParams(vmem_limit_bytes=SMALL_LIMIT),
        cost_estimate=cost(0.1, 14 * 3 * PART * AHEAD),
        name="adamw_ahead",
    )(owners, factor, g, w, mv, mv)


def place_kernel(n, owners_ref, *refs):
    out_ref = refs[-1]
    s = pl.program_id(0)
    for k in range(n):

        @pl.when(s == k)
        def _():
            out_ref[0] = refs[k][...]


def place(piece, owners, pieces, so_far, whole):
    _, l, axis, skip, count = piece
    n = len(pieces)
    block = tuple(m // count if k == axis else m for k, m in enumerate(pieces[0].shape))

    def of(k):
        return lambda s, i, own: spot(axis, jnp.where(s == k, i, jnp.where(s < k, 0, count - 1)))

    in_specs = [pl.BlockSpec(block, of(k)) for k in range(n)]
    args = list(pieces)
    aliases = {}
    if so_far is not None:
        in_specs.append(ANY)
        args.append(so_far)
        aliases = {n + 1: 0}
    return pl.pallas_call(
        functools.partial(place_kernel, n),
        grid_spec=pltpu.PrefetchScalarGridSpec(
            num_scalar_prefetch=1,
            grid=(n, count),
            in_specs=in_specs,
            out_specs=pl.BlockSpec(
                (1, *block), lambda s, i, own: (l, 3 * own[s] + skip + i, 0) if axis == 0 else (l, own[s], skip + i)
            ),
        ),
        out_shape=jax.ShapeDtypeStruct(whole.shape, BF),
        input_output_aliases=aliases,
        compiler_params=pltpu.CompilerParams(vmem_limit_bytes=SMALL_LIMIT),
        cost_estimate=cost(0.1, whole.size),
    )(owners, *args)


def place_ahead_kernel(owners_ref, new_ref, so_far, out_ref):
    out_ref[...] = new_ref[...]


def place_ahead(owners, new, so_far):
    block = (1, PART, THIRD)
    return pl.pallas_call(
        place_ahead_kernel,
        grid_spec=pltpu.PrefetchScalarGridSpec(
            num_scalar_prefetch=1,
            grid=(3, 2),
            in_specs=[pl.BlockSpec(block, lambda s, i, own: (s, 0, i)), ANY],
            out_specs=pl.BlockSpec(block, lambda s, i, own: (1, own[s], i)),
        ),
        out_shape=jax.ShapeDtypeStruct(so_far.shape, BF),
        input_output_aliases={2: 0},
        compiler_params=pltpu.CompilerParams(vmem_limit_bytes=SMALL_LIMIT),
        cost_estimate=cost(0.1, 4 * 3 * PART * AHEAD),
        name="place_ahead",
    )(owners, new, so_far)


PIECES = [(GATE, 1, 1, 2, 1)] + [(GATE, 0, 1, n, 1) for n in range(3)]
PIECES += [(n, l, 0, *part) for n, part in ((UP, (0, 3)), (DOWN, (0, 2)), (DOWN, (2, 1))) for l in range(LAYERS)]
KNOWN = (0, 1, 1, 0, 2)


def solution(mesh):
    def swap(t, mask):
        return lax.ppermute(t, "dp", [(i, i ^ mask) for i in range(8)])

    def step(x, dy, wg, wu, wd, mg, mu, md, vg, vu, vd):
        x, dy = x[0], dy[0]
        me = lax.axis_index("dp")
        a, ht, sl, q, h1, mv = forward(x, wg, wu, wd, mg, vg)
        *gradients, factor, g_ahead = backward(Lags(2, 3, 2, 2), a, dy, wd, sl, q, ht, wg, wu, h1)
        at = me[None].astype(jnp.int32)
        groups = {name: jnp.stack([me ^ k for k in group]).astype(jnp.int32) for name, group in GROUPS.items()}
        mats = ((wg, mg, vg), (wu, mu, vu), (wd, md, vd))
        moments, whole = [None] * 3, [None] * 3

        def put(kind, piece, have):
            n = piece[0]
            whole[n] = place(piece, groups[kind], [have[k] for k in GROUPS[kind]], whole[n], mats[n][0])

        def new_rows(piece):
            n = piece[0]
            new, *moments[n] = adamw(piece, at, factor, gradients[n], *mats[n], moments[n])
            return new

        everything = []
        for number, piece in enumerate(PIECES):
            have = {}
            everything.append(have)
            have[0] = new_rows(piece)
            have[4] = swap(have[0], 4)
            have[2] = swap(have[0], 2)
            have[6] = swap(have[4], 2) if number % 2 else swap(have[2], 4)
            for k in (0, 4, 2, 6):
                have[k + 1] = swap(have[k], 1)
            put("own", piece, have)
            put("near", piece, have)
        have = {0: new_rows(KNOWN)}
        have[1] = swap(have[0], 1)
        put("own", KNOWN, have)
        ahead = adamw_ahead(groups["ahead_own"], factor, g_ahead, wg, mv)
        for kind, new in (("ahead_own", ahead), ("ahead_partner", swap(ahead, 1))):
            whole[0] = place_ahead(groups[kind], new, whole[0])
        for piece, have in zip(PIECES, everything):
            put("across", piece, have)
            put("last", piece, have)
        return tuple(whole + [m[0] for m in moments] + [m[1] for m in moments])

    whole, rows = P(), P(None, "dp")
    return jax.shard_map(
        step,
        mesh=mesh,
        in_specs=(P(("rep", "dp")),) * 2 + (whole,) * 3 + (rows,) * 6,
        out_specs=(P("rep"),) * 3 + (P("rep", "dp"),) * 6,
        check_vma=False,
    )
```

```python
import functools

import jax
import jax.numpy as jnp
from jax import lax
from jax.experimental import pallas as pl
from jax.experimental.pallas import tpu as pltpu
from jax.sharding import PartitionSpec as P


BF = jnp.bfloat16
F32 = jnp.float32
MESH = pl.DeviceIdType.MESH
TOKENS, D, FF, LAYERS = 2048, 1536, 4224, 2
BLOCK = 256
STEPS = -(-FF // BLOCK)
LAST = FF - (STEPS - 1) * BLOCK
ALL = LAYERS * STEPS
PART = D // 8
SUB = BLOCK // 8
OWN_DOWN = FF // 8
LAST_SUB = OWN_DOWN - (STEPS - 1) * SUB
HALF = PART // 2
CHUNK = PART + HALF
COUNT = 3 * LAYERS * D * FF
THIRD = FF // 3
GATE, UP, DOWN = range(3)
AHEAD = 2 * THIRD
TILES = AHEAD // BLOCK
SPREAD = 13
VMEM_LIMIT = 67043328
SMALL_LIMIT = 48 << 20


ANY = pl.BlockSpec(memory_space=pl.ANY)
SQUEEZED = pl.Squeezed()
FACTOR = (8, 128)
FEW = 16
FIRST = pl.BlockSpec(FACTOR, lambda *_: (0, 0))
GROUPS = {"own": (0, 1), "near": (4, 2, 5, 3), "across": (6,), "last": (7,), "ahead_own": (4, 2, 6), "ahead_partner": (5, 3, 7)}


def dot(a, b, dims="nn"):
    ca, cb = ("tn".index(dims[0]), "nt".index(dims[1]))
    return lax.dot_general(a, b, (((ca,), (cb,)), ((), ())), preferred_element_type=F32)


def band(i, n, start=0):
    return pl.ds(pl.multiple_of(start + i * n, n), n)


def resident(shape):
    return pl.BlockSpec(shape, lambda *_: (0,) * len(shape), pipeline_mode=pl.Buffered(1))


def cost(units, bytes_accessed):
    return pl.CostEstimate(flops=int(units * 2 * TOKENS * D * FF), bytes_accessed=int(bytes_accessed), transcendentals=0)


def normed(h):
    wide = h.astype(F32)
    scale = lax.rsqrt(jnp.mean(wide * wide, -1, keepdims=True) + 1e-6)
    return (wide * scale).astype(BF)


def neighbours():
    me = lax.axis_index("dp")
    x, y, c = lax.div(me, 4), lax.rem(lax.div(me, 2), 2), lax.rem(me, 2)
    return (me, x, y, c), [{"dp": me + k * (1 - 2 * t)} for k, t in ((1, c), (4, x), (2, y))]


def remote(src, dst, send, recv, to):
    return pltpu.make_async_remote_copy(src_ref=src, dst_ref=dst, send_sem=send, recv_sem=recv, device_id=to, device_id_type=MESH)


class Weights:
    def __init__(self, l, wg, wu, wd, gu_ref, down_ref, sems):
        self.l, self.wg, self.wu, self.wd, self.gu_ref, self.down_ref, self.sems = l, wg, wu, wd, gu_ref, down_ref, sems

    def copies(self, j, last):
        slot, block, l = lax.rem(j, 2), lax.rem(j, STEPS), self.l
        if l is None:
            l = lax.div(j, STEPS)
        width = LAST if last else BLOCK
        start = (STEPS - 1) * BLOCK if last else pl.multiple_of(block * BLOCK, BLOCK)
        columns = pl.ds(start, width)
        pairs = [
            (self.wg.at[l, :, columns], self.gu_ref.at[slot, :, pl.ds(0, width)]),
            (self.wu.at[l, :, columns], self.gu_ref.at[slot, :, pl.ds(width, width)]),
        ]
        if self.wd is not None:
            pairs.append((self.wd.at[l, columns], self.down_ref.at[slot, pl.ds(0, width)]))
        return [pltpu.make_async_copy(src, dst, self.sems.at[slot, n]) for n, (src, dst) in enumerate(pairs)]

    def each(self, j, act):
        block = lax.rem(j, STEPS)

        @pl.when(block < STEPS - 1)
        def _():
            for copy in self.copies(j, False):
                act(copy)

        @pl.when(block == STEPS - 1)
        def _():
            for copy in self.copies(j, True):
                act(copy)

    def start(self, j):
        self.each(j, lambda copy: copy.start())

    def wait(self, j):
        self.each(j, lambda copy: copy.wait())


def forward_kernel(x_ref, wg, wu, wd, m_in, v_in, *refs):
    a_out, ht_ref, sl_ref, q_ref, h_out, mv_out, *refs = refs
    a_ref, h_ref, gu_ref, down_ref, hid_ref, acc_ref, w_sems, sems, near_send, near_recv, far_send, far_recv = refs
    j = pl.program_id(0)
    block = lax.rem(j, STEPS)
    weights = Weights(None, wg, wu, wd, gu_ref, down_ref, w_sems)
    _, (_, to_x, to_y) = neighbours()
    barrier = pltpu.get_barrier_semaphore()
    keep = [pltpu.make_async_copy(a_ref, a_out.at[l], sems.at[l]) for l in range(LAYERS)]
    keep_h = pltpu.make_async_copy(h_ref, h_out, sems.at[2])

    def near(k):
        src = (m_in, v_in)[k].at[1, :, pl.ds(0, AHEAD)]
        return [remote(src, mv_out.at[k, n], near_send.at[k, n], near_recv.at[k, n], to) for n, to in enumerate((to_x, to_y))]

    def far(k):
        return [
            remote(mv_out.at[k, n, rows], mv_out.at[k, 2, rows], far_send.at[k, n], far_recv.at[k, n], to)
            for n, (rows, to) in enumerate(((pl.ds(0, HALF), to_y), (pl.ds(HALF, HALF), to_x)))
        ]

    @pl.when(j == 0)
    def _():
        for to in (to_x, to_y):
            pl.semaphore_signal(barrier, inc=1, device_id=to, device_id_type=MESH)
        weights.start(j)

        @pl.loop(0, TOKENS // BLOCK)
        def _(i):
            r = band(i, BLOCK)
            a_ref[r, :] = normed(x_ref[r, :])
            acc_ref[r, :] = jnp.zeros((BLOCK, D), F32)

        keep[0].start()

    @pl.when(j == 2)
    def _():
        pl.semaphore_wait(barrier, 2)
        for k in range(2):
            for copy in near(k):
                copy.start()

    @pl.when(j == STEPS)
    def _():
        keep[0].wait()

        @pl.loop(0, TOKENS // BLOCK)
        def _(i):
            r = band(i, BLOCK)
            h = x_ref[r, :] + acc_ref[r, :].astype(BF)
            h_ref[r, :] = h
            a_ref[r, :] = normed(h)

        keep[1].start()
        keep_h.start()

    @pl.when(j == STEPS + 4)
    def _():
        for k in range(2):
            for copy in near(k):
                copy.wait()
            for copy in far(k):
                copy.start()

    pl.when(j + 1 < ALL)(lambda: weights.start(j + 1))
    weights.wait(j)
    slot = lax.rem(j, 2)

    def hidden(width):
        for i in range(TOKENS // BLOCK):
            r = slice(BLOCK * i, BLOCK * (i + 1))
            gu = dot(a_ref[r, :], gu_ref[slot, :, : 2 * width])
            g, u = gu[:, :width], gu[:, width:]
            s = jax.nn.sigmoid(g)
            sl = g * s
            sl_ref[0, r, :width] = sl
            q_ref[0, r, :width] = u * (s * (1.0 + g * (1.0 - s)))
            hid = (sl * u).astype(BF)
            hid_ref[r, :width] = hid
            ht_ref[0, :width, r] = hid.T

    pl.when(block < STEPS - 1)(lambda: hidden(BLOCK))

    @pl.when(block == STEPS - 1)
    def _():
        hidden(LAST)
        hid_ref[:, LAST:] = jnp.zeros((TOKENS, BLOCK - LAST), BF)

    @pl.when(j < STEPS)
    def _():
        acc_ref[...] += dot(hid_ref[...], down_ref[slot])

    @pl.when(j == ALL - 1)
    def _():
        keep[1].wait()
        keep_h.wait()
        for k in range(2):
            for copy in far(k):
                copy.wait()


def forward(x, wg, wu, wd, m, v):
    layer = lambda j: lax.div(j, STEPS)
    block = lambda j: lax.rem(j, STEPS)
    wide = pl.BlockSpec((1, TOKENS, BLOCK), lambda j: (layer(j), 0, block(j)))
    shape = jax.ShapeDtypeStruct
    return pl.pallas_call(
        forward_kernel,
        grid=(ALL,),
        in_specs=[resident((TOKENS, D))] + [ANY] * 5,
        out_specs=[ANY, pl.BlockSpec((1, BLOCK, TOKENS), lambda j: (layer(j), block(j), 0)), wide, wide, ANY, ANY],
        out_shape=[
            shape((LAYERS, TOKENS, D), BF),
            shape((LAYERS, FF, TOKENS), BF),
            *[shape((LAYERS, TOKENS, FF), F32)] * 2,
            shape((TOKENS, D), BF),
            shape((2, 3, PART, AHEAD), F32),
        ],
        scratch_shapes=[
            pltpu.VMEM((TOKENS, D), BF),
            pltpu.VMEM((TOKENS, D), BF),
            pltpu.VMEM((2, D, 2 * BLOCK), BF),
            pltpu.VMEM((2, BLOCK, D), BF),
            pltpu.VMEM((TOKENS, BLOCK), BF),
            pltpu.VMEM((TOKENS, D), F32),
            pltpu.SemaphoreType.DMA((2, 3)),
            pltpu.SemaphoreType.DMA((3,)),
            *[pltpu.SemaphoreType.DMA((2, 2))] * 4,
        ],
        compiler_params=pltpu.CompilerParams(vmem_limit_bytes=VMEM_LIMIT, collective_id=1, has_side_effects=True),
        cost_estimate=cost(5, 260e6),
        name="forward",
    )(x, wg, wu, wd, m, v)


def bits(o):
    return o // 4, o // 2 % 2, o % 2


class Lags:
    def __init__(self, second, third, b, e):
        self.second, self.third, self.b, self.e = second, third, b, e
        self.s = third + 1
        self.a = third + 2
        self.c = second + third
        self.d = 2 * (third - second)


def backward_kernel(lags, a_in, dy_in, wd_ref, sl_ref, q_ref, ht_ref, wg, wu, h_in, m_in, v_in, *refs):
    g_gate, g_up, g_down, f_ref, far_out, new_out, acc_ref, gu_ref, w_sems, sq_ref, every_ref, f_send, f_recv, *refs = refs
    near_send, near_recv, far_send, far_recv, a_ref, dy_ref, dgu_ref, s_ref, a2_ref, bx, by, cx, cy, ex, ey, dx, dy2, *refs = refs
    og, ou, od, s_send, a_recv, bx_send, by_send, cx_recv, cy_recv, ex_send, ey_send, dx_recv, dy_recv, out_sem, a_sem, new_sem = refs
    weights = Weights(1, wg, wu, None, gu_ref, None, w_sems)
    j = pl.program_id(0)
    block = lax.rem(j, STEPS)
    (me, x, y, c), (to_core, to_x, to_y) = neighbours()
    xn, yn, cn = (1 - k for k in (x, y, c))
    others = [{"dp": lax.rem(me + k, 8)} for k in range(1, 8)]

    def columns(last):
        return pl.ds(0, LAST if last else BLOCK)

    def pair(i, last, which=(0, 1)):
        s, a, w = lax.rem(i, lags.s), lax.rem(i, lags.a), columns(last)
        return [
            remote(s_ref.at[s, n, :, :, cn, :, w], a2_ref.at[a, n, :, :, :, w], s_send.at[s, k], a_recv.at[a, k], to_core)
            for k, n in ((k, (pl.ds(0, 2), pl.ds(2, 1))[k]) for k in which)
        ]

    def first(i, last):
        b, k, w = lax.rem(i, lags.b), lax.rem(i, lags.c), columns(last)
        return [
            remote(bx.at[b, :, :, w], cx.at[k, :, :, w], bx_send.at[b], cx_recv.at[k], to_x),
            remote(by.at[b, :, :, w], cy.at[k, :, :, w], by_send.at[b], cy_recv.at[k], to_y),
        ]

    def second(i, last):
        e, k, w = lax.rem(i, lags.e), lax.rem(i, lags.d), columns(last)
        return [
            remote(ex.at[e, :, w], dx.at[k, :, w], ex_send.at[e], dx_recv.at[k], to_x),
            remote(ey.at[e, :, w], dy2.at[k, :, w], ey_send.at[e], dy_recv.at[k], to_y),
        ]

    def outs(i, last):
        o, p, l, n = lax.rem(i, 2), lax.rem(i, og.shape[0]), 1 - lax.div(i, STEPS), lax.rem(i, STEPS)
        w = columns(last)
        wide = pl.ds(pl.multiple_of(n * BLOCK, BLOCK), w.size)
        deep = pl.ds(pl.multiple_of(n * SUB, SUB), LAST_SUB if last else SUB)
        srcs = og.at[p, :, w], ou.at[o, :, w], od.at[o, pl.ds(0, deep.size)]
        dsts = g_gate.at[l, :, wide], g_up.at[l, :, wide], g_down.at[l, deep]
        return [pltpu.make_async_copy(s, d, out_sem.at[o, n]) for n, (s, d) in enumerate(zip(srcs, dsts))]

    def each(i, copies, act):
        last = lax.rem(i, STEPS) == STEPS - 1

        @pl.when(jnp.logical_not(last))
        def _():
            for copy in copies(i, False):
                act(copy)

        @pl.when(last)
        def _():
            for copy in copies(i, True):
                act(copy)

    def start(copy):
        copy.start()

    def total(*terms):
        return functools.reduce(lambda p, q: p + q, [t.astype(F32) for t in terms])

    def take_first(i):
        each(i, pair, lambda copy: copy.wait())
        s, a, b = lax.rem(i, lags.s), lax.rem(i, lags.a), lax.rem(i, lags.b)

        pl.when(i >= lags.b)(lambda: each(i - lags.b, first, lambda copy: copy.wait_send()))

        for t in range(2):
            bx[b, t, :PART] = total(s_ref[s, GATE, xn, t, c], a2_ref[a, GATE, xn, t]).astype(BF)
            bx[b, t, PART:] = total(s_ref[s, DOWN, xn, t, c, :HALF], a2_ref[a, DOWN, xn, t, :HALF]).astype(BF)
            by[b, t, :PART] = total(s_ref[s, UP, t, yn, c], a2_ref[a, UP, t, yn]).astype(BF)
            by[b, t, PART:] = total(s_ref[s, DOWN, t, yn, c, HALF:], a2_ref[a, DOWN, t, yn, HALF:]).astype(BF)
        each(i, first, start)

    def take_second(i):
        each(i, first, lambda copy: copy.wait_recv())
        s, a, k, e = lax.rem(i, lags.s), lax.rem(i, lags.a), lax.rem(i, lags.c), lax.rem(i, lags.e)

        pl.when(i >= lags.e)(lambda: each(i - lags.e, second, lambda copy: copy.wait_send()))

        ey[e, :PART] = total(s_ref[s, GATE, x, yn, c], a2_ref[a, GATE, x, yn], cx[k, yn, :PART]).astype(BF)
        ey[e, PART:] = total(s_ref[s, DOWN, x, yn, c, :HALF], a2_ref[a, DOWN, x, yn, :HALF], cx[k, yn, PART:]).astype(BF)
        ex[e, :PART] = total(s_ref[s, UP, xn, y, c], a2_ref[a, UP, xn, y], cy[k, xn, :PART]).astype(BF)
        ex[e, PART:] = total(s_ref[s, DOWN, xn, y, c, HALF:], a2_ref[a, DOWN, xn, y, HALF:], cy[k, xn, PART:]).astype(BF)
        each(i, second, start)

    def take_third(i):
        each(i, second, lambda copy: copy.wait_recv())
        s, a, k, d, o = (lax.rem(i, n) for n in (lags.s, lags.a, lags.c, lags.d, 2))

        pl.when(i >= 1)(lambda: each(i - 1, outs, lambda copy: copy.wait()))

        gate = total(s_ref[s, GATE, x, y, c], a2_ref[a, GATE, x, y], cx[k, y, :PART], dy2[d, :PART]).astype(BF)
        up = total(s_ref[s, UP, x, y, c], a2_ref[a, UP, x, y], cy[k, x, :PART], dx[d, :PART]).astype(BF)
        og[lax.rem(i, og.shape[0])] = gate
        ou[o] = up
        low = total(s_ref[s, DOWN, x, y, c, :HALF], a2_ref[a, DOWN, x, y, :HALF], cx[k, y, PART:], dy2[d, PART:]).astype(BF)
        high = total(s_ref[s, DOWN, x, y, c, HALF:], a2_ref[a, DOWN, x, y, HALF:], cy[k, x, PART:], dx[d, PART:]).astype(BF)
        downs = [half[SUB * n : SUB * n + SUB] for half in (low, high) for n in range(HALF // SUB)]

        def squares(t):
            wide = t.astype(F32)
            return jnp.sum((wide * wide).reshape(-1, 8, t.shape[-1]), 0)

        last = lax.rem(i, STEPS) == STEPS - 1

        @pl.when(jnp.logical_not(last))
        def _():
            for n, one in enumerate(downs):
                od[o, :, BLOCK * n : BLOCK * n + BLOCK] = one
            sq_ref[...] += squares(gate) + squares(up) + squares(low) + squares(high)

        @pl.when(last)
        def _():
            for n, one in enumerate(downs):
                od[o, :LAST_SUB, BLOCK * n : BLOCK * n + LAST] = one[:LAST_SUB, :LAST]
                od[o, :LAST_SUB, BLOCK * n + LAST : BLOCK * n + BLOCK] = one[LAST_SUB:, :LAST]
            sq_ref[:, :LAST] += sum(squares(t[:, :LAST]) for t in (gate, up, low, high))

        each(i, outs, start)

    def near(t):
        k = lax.rem(t, 4)
        src = og.at[lax.rem(t, og.shape[0])]
        return [remote(src, far_out.at[n, t], near_send.at[k, n], near_recv.at[k, n], to) for n, to in enumerate((to_x, to_y))]

    def far(t):
        k = lax.rem(t, 4)
        return [
            remote(far_out.at[n, t, rows], far_out.at[2, t, rows], far_send.at[k, n], far_recv.at[k, n], to)
            for n, (rows, to) in enumerate(((pl.ds(0, HALF), to_y), (pl.ds(HALF, HALF), to_x)))
        ]

    def at_step(n, act):
        t = lax.div(n * TILES, SPREAD)

        @pl.when((n >= 0) & (n < SPREAD) & ((n == 0) | (t > lax.div((n - 1) * TILES, SPREAD))))
        def _():
            act(t)

    def pass_on(t):
        for copy in near(t):
            copy.wait()
        for copy in far(t):
            copy.start()

    take_a1, take_a0 = (pltpu.make_async_copy(a_in.at[l], a_ref, a_sem.at[l]) for l in (1, 0))
    take_h = pltpu.make_async_copy(h_in, a_ref, a_sem.at[2])
    take_dy = pltpu.make_async_copy(dy_in, dy_ref, a_sem.at[3])
    barrier = pltpu.get_barrier_semaphore()

    @pl.when(j == 0)
    def _():
        take_dy.start()
        take_a1.start()
        weights.start(j)
        for to in others:
            pl.semaphore_signal(barrier, inc=1, device_id=to, device_id_type=MESH)
        sq_ref[...] = jnp.zeros_like(sq_ref)

        @pl.loop(0, TOKENS // BLOCK)
        def _(i):
            acc_ref[band(i, BLOCK), :] = jnp.zeros((BLOCK, D), F32)

        take_dy.wait()

    @pl.when(j == STEPS)
    def _():
        take_h.wait()

        @pl.loop(0, TOKENS // LAST)
        def _(i):
            r = band(i, LAST)
            h = a_ref[r, :].astype(F32)
            da = acc_ref[r, :].astype(BF).astype(F32)
            scale = lax.rsqrt(jnp.mean(h * h, -1, keepdims=True) + 1e-6)
            along = jnp.sum(da * h, -1, keepdims=True) * (scale * scale * scale) * (1.0 / D)
            dy_ref[r, :] = dy_ref[r, :] + (da * scale - h * along).astype(BF)

        take_a0.start()

    @pl.when(j < ALL)
    def _():
        pl.when(j + 1 < STEPS)(lambda: weights.start(j + 1))
        s = lax.rem(j, lags.s)
        for i in range(4):
            r = slice(2 * BLOCK * i, 2 * BLOCK * (i + 1))
            dh = dot(dy_ref[r, :], wd_ref[0], "nt").astype(BF).astype(F32)
            dgu_ref[r, :BLOCK] = (dh * q_ref[0, r, :]).astype(BF)
            dgu_ref[r, BLOCK:] = (dh * sl_ref[0, r, :]).astype(BF)

        pl.when(j == 0)(lambda: take_a1.wait())
        pl.when(j == STEPS)(lambda: take_a0.wait())

        def gate_up(width):
            for h in range(2):
                gu = dot(a_ref[:, D // 2 * h : D // 2 * (h + 1)], dgu_ref[:, : 2 * width], "tn")
                for o in range(4):
                    for t in range(2):
                        s_ref[s, t, h, o // 2, o % 2, :, :width] = gu[PART * o : PART * o + PART, width * t : width * t + width].astype(BF)

        pl.when(block < STEPS - 1)(lambda: gate_up(BLOCK))

        @pl.when(block == STEPS - 1)
        def _():
            dgu_ref[:, LAST:BLOCK] = dgu_ref[:, BLOCK : BLOCK + LAST]
            gate_up(LAST)

        pl.when(j == STEPS - 1)(lambda: take_h.start())
        pl.when(j == 0)(lambda: pl.semaphore_wait(barrier, len(others)))
        each(j, functools.partial(pair, which=(0,)), start)
        for h in range(2):
            down = dot(ht_ref[...].reshape(BLOCK, TOKENS), dy_ref[:, D // 2 * h : D // 2 * (h + 1)])
            for o in range(8):
                for n in range(3):
                    s_ref[(s, DOWN, *bits(o), slice(SUB * (3 * h + n), SUB * (3 * h + n + 1)))] = down[
                        SUB * o : SUB * o + SUB, BLOCK * n : BLOCK * n + BLOCK
                    ].astype(BF)

        @pl.when(block == STEPS - 1)
        def _():
            for o in range(8):
                for n in range(6):
                    half = SUB * n + LAST_SUB
                    s_ref[(s, DOWN, *bits(o), slice(half, SUB * n + SUB), slice(LAST))] = s_ref[
                        (s, DOWN, *bits(o), slice(SUB * n, half), slice(LAST, BLOCK))
                    ]

        each(j, functools.partial(pair, which=(1,)), start)

        def add_da(width):
            weights.wait(j)
            for i in range(8):
                r = slice(BLOCK * i, BLOCK * (i + 1))
                acc_ref[r, :] += dot(dgu_ref[r, : 2 * width], gu_ref[lax.rem(j, 2), :, : 2 * width], "nt")

        pl.when(j < STEPS - 1)(lambda: add_da(BLOCK))
        pl.when(j == STEPS - 1)(lambda: add_da(LAST))

    pl.when((j >= lags.third) & (j < ALL + lags.third))(lambda: take_third(j - lags.third))
    pl.when((j >= lags.second) & (j < ALL + lags.second))(lambda: take_second(j - lags.second))
    pl.when(j < ALL)(lambda: take_first(j))
    at_step(j - lags.third - 4, lambda t: [copy.wait() for copy in far(t)])
    at_step(j - lags.third - 2, pass_on)
    at_step(j - lags.third, lambda t: [copy.start() for copy in near(t)])

    chunks = [(k, start, min(2 * BLOCK, THIRD - start)) for k, start in enumerate(range(0, THIRD, 2 * BLOCK))]

    def rows_of(k):
        return pl.ds(PART * k, PART)

    def gathered():
        mine = band(me, PART)
        copies = [(t.at[1, :, pl.ds(AHEAD, THIRD)], acc_ref.at[rows_of(k), pl.ds(0, THIRD)]) for k, t in enumerate((m_in, v_in))]
        for k, start, width in chunks:
            w, room = pl.ds(AHEAD + start, width), (rows_of(k), pl.ds(0, width))
            copies += [(wg.at[1, mine, w], gu_ref.at[(0, *room)]), (g_gate.at[1, :, w], gu_ref.at[(1, *room)])]
        return [pltpu.make_async_copy(src, dst, new_sem.at[n]) for n, (src, dst) in enumerate(copies)]

    def given():
        return [
            pltpu.make_async_copy(gu_ref.at[0, rows_of(k), pl.ds(0, width)], new_out.at[:, pl.ds(start, width)], new_sem.at[k])
            for k, start, width in chunks
        ]

    @pl.when(j == ALL)
    def _():
        for copy in gathered():
            copy.start()

    @pl.when(j == ALL + lags.third - 1)
    def _():
        for copy in gathered():
            copy.wait()
        both = sq_ref[...]
        every_ref[me] = both[:, :128] + both[:, 128:]

        def exchange():
            return [remote(every_ref.at[me], every_ref.at[me], f_send.at[n], f_recv.at[n], to) for n, to in enumerate(others)]

        for copy in exchange():
            copy.start()
        for i in range(ALL - lags.b, ALL):
            for copy in first(jnp.int32(i), i == ALL - 1):
                copy.wait_send()
        for i in range(ALL - lags.e, ALL):
            for copy in second(jnp.int32(i), i == ALL - 1):
                copy.wait_send()
        for copy in outs(jnp.int32(ALL - 1), True):
            copy.wait()
        for copy in exchange():
            copy.wait()
        squares = functools.reduce(lambda p, q: p + q, [every_ref[n] for n in range(8)])
        squares = jnp.sum(jnp.sum(squares, axis=1, keepdims=True), axis=0, keepdims=True)
        factor = jnp.minimum(1.0, 0.5 * lax.rsqrt(squares / COUNT + 1e-30))
        f_ref[...] = jnp.broadcast_to(factor, FACTOR)

        @pl.loop(0, PART // FEW)
        def _(i):
            for k, start, width in chunks:
                r, w = band(i, FEW, PART * k), pl.ds(start, width)
                m, v = (acc_ref[band(i, FEW, PART * n), w] for n in range(2))
                gu_ref[0, r, :width], _, _ = stepped(factor, gu_ref[1, r, :width], gu_ref[0, r, :width], m, v)

        for copy in given():
            copy.start()
        for copy in given():
            copy.wait()


def backward(lags, a, dy, wd, sl, q, ht, wg, wu, h, m, v):
    layer = lambda j: 1 - lax.div(jnp.minimum(j, ALL - 1), STEPS)
    block = lambda j: lax.rem(jnp.minimum(j, ALL - 1), STEPS)
    wide = pl.BlockSpec((1, TOKENS, BLOCK), lambda j: (layer(j), 0, block(j)))
    shape = jax.ShapeDtypeStruct
    piece = (PART, BLOCK)
    dma = pltpu.SemaphoreType.DMA
    return pl.pallas_call(
        functools.partial(backward_kernel, lags),
        grid=(ALL + lags.third,),
        in_specs=[
            ANY,
            ANY,
            pl.BlockSpec((1, BLOCK, D), lambda j: (layer(j), block(j), 0)),
            wide,
            wide,
            pl.BlockSpec((8, SUB, TOKENS), lambda j: (layer(j), block(j), 0)),
            *[ANY] * 5,
        ],
        out_specs=[ANY, ANY, ANY, FIRST, ANY, ANY],
        out_shape=[
            *[shape((LAYERS, PART, FF), BF)] * 2,
            shape((LAYERS, OWN_DOWN, D), BF),
            shape(FACTOR, F32),
            shape((3, TILES, *piece), BF),
            shape((PART, THIRD), BF),
        ],
        scratch_shapes=[
            pltpu.VMEM((TOKENS, D), F32),
            pltpu.VMEM((2, D, 2 * BLOCK), BF),
            dma((2, 3)),
            pltpu.VMEM((8, BLOCK), F32),
            pltpu.VMEM((8, *FACTOR), F32),
            *[dma((7,))] * 2,
            *[dma((4, 2))] * 4,
            *[pltpu.VMEM((TOKENS, D), BF)] * 2,
            pltpu.VMEM((TOKENS, 2 * BLOCK), BF),
            pltpu.VMEM((lags.s, 3, 2, 2, 2, *piece), BF),
            pltpu.VMEM((lags.a, 3, 2, 2, *piece), BF),
            *[pltpu.VMEM((n, 2, CHUNK, BLOCK), BF) for n in (lags.b, lags.b, lags.c, lags.c)],
            *[pltpu.VMEM((n, CHUNK, BLOCK), BF) for n in (lags.e, lags.e, lags.d, lags.d)],
            *[pltpu.VMEM((n, *piece), BF) for n in (5, 2)],
            pltpu.VMEM((2, SUB, D), BF),
            *[dma((n, 2)) for n in (lags.s, lags.a)],
            *[dma((n,)) for n in (lags.b, lags.b, lags.c, lags.c, lags.e, lags.e, lags.d, lags.d)],
            dma((2, 3)),
            dma((4,)),
            dma((8,)),
        ],
        compiler_params=pltpu.CompilerParams(vmem_limit_bytes=VMEM_LIMIT, collective_id=0, has_side_effects=True),
        cost_estimate=cost(10, 300e6),
        name="backward",
    )(a, dy, wd, sl, q, ht.reshape(LAYERS * 8, OWN_DOWN, TOKENS), wg, wu, h, m, v)


def stepped(factor, g, w, m, v):
    g, w = g.astype(F32) * factor, w.astype(F32)
    m = 0.9 * m + 0.1 * g
    v = 0.95 * v + 0.05 * g * g
    return (w - 0.02 * (m * lax.rsqrt(v + 1e-8) + 0.1 * w)).astype(BF), m, v


def adamw_kernel(at_ref, f_ref, g_ref, w_ref, m_ref, v_ref, *refs):
    nw_ref, nm_ref, nv_ref = refs[-3:]
    factor = f_ref[:1, :1]

    @pl.loop(0, g_ref.shape[0] // FEW)
    def _(i):
        r = band(i, FEW)
        nw_ref[r, :], nm_ref[0, r, :], nv_ref[0, r, :] = stepped(factor, g_ref[r, :], w_ref[0, r, :], m_ref[0, r, :], v_ref[0, r, :])


def thirds(shape, axis):
    return tuple(n // 3 if k == axis else n for k, n in enumerate(shape))


def spot(axis, i, other=0):
    return (i, other) if axis == 0 else (other, i)


def adamw(piece, at, factor, g, w, m, v, so_far=None):
    _, l, axis, skip, count = piece
    block = thirds(g.shape[1:], axis)
    moment = pl.BlockSpec((1, *block), lambda i, at: (l, *spot(axis, skip + i)))
    in_specs = [
        FIRST,
        pl.BlockSpec((SQUEEZED, *block), lambda i, at: (l, *spot(axis, skip + i))),
        pl.BlockSpec((1, *block), lambda i, at: (l, 3 * at[0] + skip + i, 0) if axis == 0 else (l, at[0], skip + i)),
        moment,
        moment,
    ]
    args = [factor, g, w, m, v]
    aliases = {}
    if so_far is not None:
        in_specs += [ANY, ANY]
        args += so_far
        aliases = {6: 1, 7: 2}
    new = tuple(n * count if k == axis else n for k, n in enumerate(block))
    return pl.pallas_call(
        adamw_kernel,
        grid_spec=pltpu.PrefetchScalarGridSpec(
            num_scalar_prefetch=1,
            grid=(count,),
            in_specs=in_specs,
            out_specs=[pl.BlockSpec(block, lambda i, at: spot(axis, i)), moment, moment],
        ),
        out_shape=[jax.ShapeDtypeStruct(new, BF)] + [jax.ShapeDtypeStruct(m.shape, F32)] * 2,
        input_output_aliases=aliases,
        compiler_params=pltpu.CompilerParams(vmem_limit_bytes=SMALL_LIMIT),
        cost_estimate=cost(0.1, m.size),
    )(at, *args)


def adamw_ahead_kernel(owners_ref, f_ref, g_ref, w_ref, m_ref, v_ref, nw_ref):
    factor = f_ref[:1, :1]

    @pl.loop(0, PART // SUB)
    def _(i):
        r = band(i, SUB)
        nw_ref[0, r, :], _, _ = stepped(factor, g_ref[r, :], w_ref[0, r, :], m_ref[r, :], v_ref[r, :])


def adamw_ahead(owners, factor, g, w, mv):
    block = (PART, BLOCK)
    return pl.pallas_call(
        adamw_ahead_kernel,
        grid_spec=pltpu.PrefetchScalarGridSpec(
            num_scalar_prefetch=1,
            grid=(3, TILES),
            in_specs=[
                FIRST,
                pl.BlockSpec((SQUEEZED, SQUEEZED, *block), lambda s, t, own: (s, t, 0, 0)),
                pl.BlockSpec((1, *block), lambda s, t, own: (1, own[s], t)),
                *[pl.BlockSpec((SQUEEZED, SQUEEZED, *block), lambda s, t, own, k=k: (k, s, 0, t)) for k in range(2)],
            ],
            out_specs=pl.BlockSpec((1, *block), lambda s, t, own: (s, 0, t)),
        ),
        out_shape=jax.ShapeDtypeStruct((3, PART, AHEAD), BF),
        compiler_params=pltpu.CompilerParams(vmem_limit_bytes=SMALL_LIMIT),
        cost_estimate=cost(0.1, 14 * 3 * PART * AHEAD),
        name="adamw_ahead",
    )(owners, factor, g, w, mv, mv)


def place_kernel(n, owners_ref, *refs):
    out_ref = refs[-1]
    s = pl.program_id(0)
    for k in range(n):

        @pl.when(s == k)
        def _():
            out_ref[0] = refs[k][...]


def place(piece, owners, pieces, so_far, whole, both=False):
    _, l, axis, skip, count = piece
    n = len(pieces)
    of_layer = lambda s: s if both else l
    block = tuple(m // count if k == axis else m for k, m in enumerate(pieces[0].shape))

    def of(k):
        return lambda s, i, own: spot(axis, jnp.where(s == k, i, jnp.where(s < k, 0, count - 1)))

    in_specs = [pl.BlockSpec(block, of(k)) for k in range(n)]
    args = list(pieces)
    aliases = {}
    if so_far is not None:
        in_specs.append(ANY)
        args.append(so_far)
        aliases = {n + 1: 0}
    return pl.pallas_call(
        functools.partial(place_kernel, n),
        grid_spec=pltpu.PrefetchScalarGridSpec(
            num_scalar_prefetch=1,
            grid=(n, count),
            in_specs=in_specs,
            out_specs=pl.BlockSpec(
                (1, *block), lambda s, i, own: (of_layer(s), 3 * own[s] + skip + i, 0) if axis == 0 else (of_layer(s), own[s], skip + i)
            ),
        ),
        out_shape=jax.ShapeDtypeStruct(whole.shape, BF),
        input_output_aliases=aliases,
        compiler_params=pltpu.CompilerParams(vmem_limit_bytes=SMALL_LIMIT),
        cost_estimate=cost(0.1, whole.size),
    )(owners, *args)


def place_ahead_kernel(owners_ref, new_ref, so_far, out_ref):
    out_ref[...] = new_ref[...]


def place_ahead(owners, new, so_far):
    block = (1, PART, THIRD)
    return pl.pallas_call(
        place_ahead_kernel,
        grid_spec=pltpu.PrefetchScalarGridSpec(
            num_scalar_prefetch=1,
            grid=(3, 2),
            in_specs=[pl.BlockSpec(block, lambda s, i, own: (s, 0, i)), ANY],
            out_specs=pl.BlockSpec(block, lambda s, i, own: (1, own[s], i)),
        ),
        out_shape=jax.ShapeDtypeStruct(so_far.shape, BF),
        input_output_aliases={2: 0},
        compiler_params=pltpu.CompilerParams(vmem_limit_bytes=SMALL_LIMIT),
        cost_estimate=cost(0.1, 4 * 3 * PART * AHEAD),
        name="place_ahead",
    )(owners, new, so_far)


PIECES = [(GATE, 1, 1, 2, 1)] + [(GATE, 0, 1, n, 1) for n in range(3)]
PIECES += [(n, l, 0, *part) for n, part in ((UP, (0, 3)), (DOWN, (0, 2)), (DOWN, (2, 1))) for l in range(LAYERS)]
KNOWN = (0, 1, 1, 0, 2)


def solution(mesh):
    def swap(t, mask):
        return lax.ppermute(t, "dp", [(i, i ^ mask) for i in range(8)])

    def step(x, dy, wg, wu, wd, mg, mu, md, vg, vu, vd):
        x, dy = x[0], dy[0]
        me = lax.axis_index("dp")
        a, ht, sl, q, h1, mv = forward(x, wg, wu, wd, mg, vg)
        *gradients, factor, g_ahead, early = backward(Lags(2, 3, 2, 2), a, dy, wd, sl, q, ht, wg, wu, h1, mg, vg)
        at = me[None].astype(jnp.int32)
        groups = {name: jnp.stack([me ^ k for k in group]).astype(jnp.int32) for name, group in GROUPS.items()}
        mats = ((wg, mg, vg), (wu, mu, vu), (wd, md, vd))
        moments, whole = [None] * 3, [None] * 3

        def put(kind, piece, have):
            n = piece[0]
            whole[n] = place(piece, groups[kind], [have[k] for k in GROUPS[kind]], whole[n], mats[n][0])

        def new_rows(piece):
            n = piece[0]
            new, *moments[n] = adamw(piece, at, factor, gradients[n], *mats[n], moments[n])
            return new

        everything = []
        for number, piece in enumerate(PIECES):
            have = {}
            everything.append(have)
            have[0] = new_rows(piece) if number else early
            have[4] = swap(have[0], 4)
            have[2] = swap(have[0], 2)
            have[6] = swap(have[4], 2) if number % 2 else swap(have[2], 4)
            for k in (0, 4, 2, 6):
                have[k + 1] = swap(have[k], 1)
            put("own", piece, have)
            put("near", piece, have)
        have = {0: new_rows(KNOWN)}
        new_rows(PIECES[0])
        have[1] = swap(have[0], 1)
        put("own", KNOWN, have)
        ahead = adamw_ahead(groups["ahead_own"], factor, g_ahead, wg, mv)
        for kind, new in (("ahead_own", ahead), ("ahead_partner", swap(ahead, 1))):
            whole[0] = place_ahead(groups[kind], new, whole[0])
        for number, (piece, have) in enumerate(zip(PIECES, everything)):
            if piece[0] == GATE:
                put("across", piece, have)
                put("last", piece, have)
            elif piece[1] == 0:
                for kind in ("across", "last"):
                    k, n = GROUPS[kind][0], piece[0]
                    pair = [have[k], everything[number + 1][k]]
                    whole[n] = place(piece, jnp.tile(groups[kind], 2), pair, whole[n], mats[n][0], both=True)
        return tuple(whole + [m[0] for m in moments] + [m[1] for m in moments])

    whole, rows = P(), P(None, "dp")
    return jax.shard_map(
        step,
        mesh=mesh,
        in_specs=(P(("rep", "dp")),) * 2 + (whole,) * 3 + (rows,) * 6,
        out_specs=(P("rep"),) * 3 + (P("rep", "dp"),) * 6,
        check_vma=False,
    )
```
